32 devices in a mesh: dp: 4 (over y, z), ep: 8 (over x, core).
Axes of the slice: x: 4, y: 2, z: 2, core: 2. Of those that a mesh axis runs over, the one named last changes fastest.
The devices are a block of a 4x4x8 slice.
Arguments:
- tokens: bfloat16 [96, 128, 2048], P(('dp', 'ep')), parts along dimension 0
- w_query: bfloat16 [2048, 32, 128], P('ep')
- w_key: bfloat16 [2048, 32, 128], P('ep')
- w_value: bfloat16 [2048, 32, 128], P('ep')
- w_out: bfloat16 [4096, 2048], P('ep')
- w_router: float32 [2048, 128], replicated
- w_one: bfloat16 [128, 2048, 768], P('ep')
- w_three: bfloat16 [128, 2048, 768], P('ep')
- w_two: bfloat16 [128, 768, 2048], P('ep')
- expert_ids: int32 [96, 128, 8], P(('dp', 'ep')), parts along dimension 0
Outputs:
- output: bfloat16 [96, 128, 2048], P(('dp', 'ep')), parts along dimension 0
There are 4 independent parts. The reference program is written for one: setup_inputs(seed, part) draws one part's arguments, and reference() takes and returns one part's arrays. A program takes and returns all parts, laid end to end along the dimension named above; an argument that names none is the same for every part.
All inputs are finite; a program needn't handle non-finite values.
Results may differ from the reference program's by a relative error of at most 0.0104012.
Values are sent between devices in bfloat16 or wider.
A program may use at most 768 MiB of HBM per device.

```python
import jax
import jax.numpy as jnp
import numpy as np
from jax import lax

D = 2048
HEADS = 32
HEAD = 128
EXPERTS = 128
TOP = 8
FF = 768
TOK_DEV = 384
SEQ = 128
GROUP = 8

TOKENS = TOK_DEV * GROUP
N_SEQ = TOKENS // SEQ
CAP = 2 * TOK_DEV * TOP // EXPERTS
WIDTH = HEADS * HEAD
EPS = 1e-6


def draw_routing(route_key):
    mean_load = TOK_DEV * TOP // EXPERTS
    ranks = np.arange(EXPERTS)
    loads = np.where(ranks < EXPERTS // 4, 2 * mean_load, np.where(ranks < EXPERTS // 2, mean_load, mean_load // 2))
    rank_of_pos = np.repeat(ranks, loads)
    order_key, device_key = jax.random.split(route_key)
    expert_order = jax.random.permutation(order_key, EXPERTS)
    grid = expert_order[rank_of_pos].reshape(TOP, TOK_DEV).T

    def one_device(dev_key):
        perm_key, shift_key = jax.random.split(dev_key)
        token_order = jax.random.permutation(perm_key, TOK_DEV)
        shift = jax.random.randint(shift_key, (TOK_DEV, 1), 0, TOP)
        columns = (jnp.arange(TOP)[None, :] + shift) % TOP
        return jnp.take_along_axis(grid[token_order], columns, axis=1)

    routes = jax.vmap(one_device)(jax.random.split(device_key, GROUP))
    return routes.reshape(N_SEQ, SEQ, TOP).astype(jnp.int32)


def setup_inputs(seed: int = 0, part: int = 0) -> dict:
    root_key = jax.random.key(seed)
    part_keys = jax.random.split(jax.random.fold_in(root_key, part), 3)
    weight_keys = jax.random.split(root_key, 8)

    def gaussian(index, shape, scale):
        return scale * jax.random.normal(weight_keys[index], shape, jnp.float32)

    seq_base = jax.random.normal(part_keys[0], (N_SEQ, 1, D), jnp.float32)
    noise = jax.random.normal(part_keys[1], (N_SEQ, SEQ, D), jnp.float32)
    return {
        'tokens': (0.6 * seq_base + 0.8 * noise).astype(jnp.bfloat16),
        'w_query': gaussian(0, (D, HEADS, HEAD), 1.5 * D ** -0.5).astype(jnp.bfloat16),
        'w_key': gaussian(1, (D, HEADS, HEAD), 1.5 * D ** -0.5).astype(jnp.bfloat16),
        'w_value': gaussian(2, (D, HEADS, HEAD), D ** -0.5).astype(jnp.bfloat16),
        'w_out': gaussian(3, (WIDTH, D), WIDTH ** -0.5).astype(jnp.bfloat16),
        'w_router': gaussian(4, (D, EXPERTS), D ** -0.5),
        'w_one': gaussian(5, (EXPERTS, D, FF), D ** -0.5).astype(jnp.bfloat16),
        'w_three': gaussian(6, (EXPERTS, D, FF), D ** -0.5).astype(jnp.bfloat16),
        'w_two': gaussian(7, (EXPERTS, FF, D), 2.0 * FF ** -0.5).astype(jnp.bfloat16),
        'expert_ids': draw_routing(part_keys[2]),
    }


def rms_norm(vals):
    wide = vals.astype(jnp.float32)
    return wide * lax.rsqrt(jnp.mean(wide * wide, axis=-1, keepdims=True) + EPS)


def reference(tokens, w_query, w_key, w_value, w_out, w_router, w_one, w_three, w_two, expert_ids):
    flat_query = w_query.reshape(D, WIDTH)
    flat_key = w_key.reshape(D, WIDTH)
    flat_value = w_value.reshape(D, WIDTH)
    causal = jnp.arange(SEQ)[:, None] >= jnp.arange(SEQ)[None, :]

    def one_sequence(seq_tokens):
        normed = rms_norm(seq_tokens).astype(jnp.bfloat16)
        query = jnp.dot(normed, flat_query, preferred_element_type=jnp.float32).astype(jnp.bfloat16)
        keys = jnp.dot(normed, flat_key, preferred_element_type=jnp.float32).astype(jnp.bfloat16)
        values = jnp.dot(normed, flat_value, preferred_element_type=jnp.float32).astype(jnp.bfloat16)
        query = query.astype(jnp.float32).reshape(SEQ, HEADS, HEAD)
        keys = keys.astype(jnp.float32).reshape(SEQ, HEADS, HEAD)
        values = values.astype(jnp.float32).reshape(SEQ, HEADS, HEAD)
        scores = jnp.einsum('qhk,shk->hqs', query, keys) * HEAD ** -0.5
        scores = jnp.where(causal, scores, -jnp.inf)
        attn_weights = jax.nn.softmax(scores, axis=-1).astype(jnp.bfloat16).astype(jnp.float32)
        context = jnp.einsum('hqs,shk->qhk', attn_weights, values).astype(jnp.bfloat16)
        attn_out = jnp.dot(context.reshape(SEQ, WIDTH), w_out, preferred_element_type=jnp.float32)
        return (seq_tokens.astype(jnp.float32) + attn_out).astype(jnp.bfloat16)

    hidden = lax.map(one_sequence, tokens).reshape(TOKENS, D)
    normed = rms_norm(hidden)
    logits = jnp.dot(normed, w_router, preferred_element_type=jnp.float32)
    ids_flat = expert_ids.reshape(TOKENS, TOP)
    gates = jax.nn.softmax(jnp.take_along_axis(logits, ids_flat, axis=1), axis=-1)
    padded = jnp.concatenate([normed.astype(jnp.bfloat16), jnp.zeros((1, D), jnp.bfloat16)], axis=0)
    limit = GROUP * CAP

    def one_expert(total_mix, expert_pack):
        expert, first_w, third_w, second_w = expert_pack
        match = ids_flat == expert
        weight = jnp.sum(jnp.where(match, gates, 0.0), axis=1)
        rows = jnp.nonzero(jnp.any(match, axis=1), size=limit, fill_value=TOKENS)[0]
        picked = padded[rows]
        first = jnp.dot(picked, first_w, preferred_element_type=jnp.float32)
        third = jnp.dot(picked, third_w, preferred_element_type=jnp.float32)
        activated = (jax.nn.silu(first) * third).astype(jnp.bfloat16)
        result = jnp.dot(activated, second_w, preferred_element_type=jnp.float32).astype(jnp.bfloat16)
        scale = jnp.concatenate([weight, jnp.zeros((1,), jnp.float32)])[rows]
        total_mix = total_mix.at[rows].add(scale[:, None] * result.astype(jnp.float32), mode='drop')
        return total_mix, None

    total_mix, _ = lax.scan(one_expert, jnp.zeros((TOKENS, D), jnp.float32), (jnp.arange(EXPERTS), w_one, w_three, w_two))
    layer_out = (hidden.astype(jnp.float32) + total_mix).astype(jnp.bfloat16)
    return layer_out.reshape(N_SEQ, SEQ, D)
```

```python
import functools

import jax
import jax.numpy as jnp
from jax import lax
from jax.experimental import pallas as pl
from jax.experimental.pallas import tpu as pltpu
from jax.sharding import PartitionSpec as P

EPS = 1e-6
SLOT = 16


def rms_norm(vals):
    wide = vals.astype(jnp.float32)
    return wide * lax.rsqrt(jnp.mean(wide * wide, axis=-1, keepdims=True) + EPS)


def attention_layer(tokens, w_query, w_key, w_value, w_out):
    seq_count = tokens.shape[0]
    seq_len = tokens.shape[1]
    head_dim = w_query.shape[2]
    normed = rms_norm(tokens).astype(jnp.bfloat16)
    query = jnp.einsum('bsd,dhk->bshk', normed, w_query, preferred_element_type=jnp.float32).astype(jnp.bfloat16)
    keys = jnp.einsum('bsd,dhk->bshk', normed, w_key, preferred_element_type=jnp.float32).astype(jnp.bfloat16)
    values = jnp.einsum('bsd,dhk->bshk', normed, w_value, preferred_element_type=jnp.float32).astype(jnp.bfloat16)
    scores = jnp.einsum('bqhk,bshk->bhqs', query, keys, preferred_element_type=jnp.float32) * head_dim ** -0.5
    causal = lax.broadcasted_iota(jnp.int32, (seq_len, seq_len), 0) >= lax.broadcasted_iota(jnp.int32, (seq_len, seq_len), 1)
    attn_weights = jax.nn.softmax(jnp.where(causal, scores, -jnp.inf), axis=-1).astype(jnp.bfloat16)
    context = jnp.einsum('bhqs,bshk->bqhk', attn_weights, values, preferred_element_type=jnp.float32).astype(jnp.bfloat16)
    attn_out = jnp.einsum('crd,de->cre', context.reshape(seq_count, seq_len, -1), w_out, preferred_element_type=jnp.float32)
    return (tokens.astype(jnp.float32) + attn_out).astype(jnp.bfloat16)


def slot_table(ids_flat, experts):
    tok_count = ids_flat.shape[0]
    member = jnp.any(ids_flat[:, :, None] == jnp.arange(experts, dtype=jnp.int32), axis=1)
    strict = lax.broadcasted_iota(jnp.int32, (tok_count, tok_count), 0) > lax.broadcasted_iota(jnp.int32, (tok_count, tok_count), 1)
    before = jnp.dot(strict.astype(jnp.bfloat16), member.astype(jnp.bfloat16), preferred_element_type=jnp.float32)
    return member, jnp.where(member, before.astype(jnp.int32), -1)


def dense_gates(hidden, w_router, member):
    normed = rms_norm(hidden)
    logits = jnp.dot(normed, w_router, precision=lax.Precision.HIGHEST, preferred_element_type=jnp.float32)
    top = jnp.max(jnp.where(member, logits, -jnp.inf), axis=1, keepdims=True)
    grown = jnp.where(member, jnp.exp(jnp.where(member, logits, top) - top), 0.0)
    return normed.astype(jnp.bfloat16), grown / jnp.sum(grown, axis=1, keepdims=True)


def dispatch_kernel(pos_ref, u_ref, out_ref, hot_ref):
    owned, toks = pos_ref.shape[1], pos_ref.shape[2]
    parts = out_ref.shape[1]
    cap = parts * SLOT
    lane = lax.broadcasted_iota(jnp.int32, (cap, toks), 0)
    for e in range(owned):
        hot_ref[e * cap:(e + 1) * cap, :] = jnp.where(lane == pos_ref[0, e:e + 1, :], 1.0, 0.0).astype(jnp.bfloat16)
    width = 512
    for c in range(u_ref.shape[1] // width):
        cols = slice(c * width, (c + 1) * width)
        rows = jnp.dot(hot_ref[...], u_ref[:, cols], preferred_element_type=jnp.float32).astype(jnp.bfloat16)
        out_ref[:, :, 0, :, cols] = rows.reshape(owned, parts, SLOT, width)


def dispatch(pos, u_all, parts):
    n, owned, toks = pos.shape
    dim = u_all.shape[1]
    return pl.pallas_call(
        dispatch_kernel,
        grid=(n,),
        in_specs=[pl.BlockSpec((1, owned, toks), lambda s: (s, 0, 0)), pl.BlockSpec((toks, dim), lambda s: (s, 0))],
        out_specs=pl.BlockSpec((owned, parts, 1, SLOT, dim), lambda s: (0, 0, s, 0, 0)),
        out_shape=jax.ShapeDtypeStruct((owned, parts, n, SLOT, dim), jnp.bfloat16),
        scratch_shapes=[pltpu.VMEM((owned * parts * SLOT, toks), jnp.bfloat16)],
        compiler_params=pltpu.CompilerParams(vmem_limit_bytes=60 * 2 ** 20),
        cost_estimate=pl.CostEstimate(flops=2 * n * owned * parts * SLOT * toks * dim, bytes_accessed=40_000_000, transcendentals=0),
        name="dispatch",
    )(pos, u_all)


def ffn_kernel(need_ref, rows_ref, one_ref, three_ref, two_ref, out_ref):
    parts, n = rows_ref.shape[1], rows_ref.shape[2]
    dim = rows_ref.shape[4]
    step = n * SLOT
    need = need_ref[pl.program_id(0)]
    for used in range(parts + 1):
        @pl.when(need == used)
        def _():
            if used:
                rows = rows_ref[0, :used].reshape(used * step, dim)
                first = jnp.dot(rows, one_ref[0], preferred_element_type=jnp.float32)
                third = jnp.dot(rows, three_ref[0], preferred_element_type=jnp.float32)
                acted = (jax.nn.silu(first) * third).astype(jnp.bfloat16)
                done = jnp.dot(acted, two_ref[0], preferred_element_type=jnp.float32).astype(jnp.bfloat16)
                out_ref[0, :used] = done.reshape(used, n, SLOT, dim)
            if used < parts:
                out_ref[0, used:] = jnp.zeros((parts - used, n, SLOT, dim), jnp.bfloat16)


def ffn(need, rows, w_one, w_three, w_two):
    owned, parts, n, _, dim = rows.shape
    inner = w_one.shape[2]
    tile = pl.BlockSpec((1, parts, n, SLOT, dim), lambda e, _: (e, 0, 0, 0, 0))
    return pl.pallas_call(
        ffn_kernel,
        grid_spec=pltpu.PrefetchScalarGridSpec(
            num_scalar_prefetch=1,
            grid=(owned,),
            in_specs=[
                tile,
                pl.BlockSpec((1, dim, inner), lambda e, _: (e, 0, 0)),
                pl.BlockSpec((1, dim, inner), lambda e, _: (e, 0, 0)),
                pl.BlockSpec((1, inner, dim), lambda e, _: (e, 0, 0)),
            ],
            out_specs=tile,
        ),
        out_shape=jax.ShapeDtypeStruct(rows.shape, jnp.bfloat16),
        compiler_params=pltpu.CompilerParams(vmem_limit_bytes=60 * 2 ** 20),
        cost_estimate=pl.CostEstimate(flops=6 * rows.size * inner, bytes_accessed=200_000_000, transcendentals=0),
        name="ffn",
    )(need, rows, w_one, w_three, w_two)


def combine_kernel(pos_ref, gate_ref, done_ref, out_ref, big_ref, mid_ref, low_ref):
    owned, toks = pos_ref.shape[1], pos_ref.shape[2]
    parts = done_ref.shape[1]
    cap = parts * SLOT
    lane = lax.broadcasted_iota(jnp.int32, (cap, toks), 0)
    gate = gate_ref[0]
    big = gate.astype(jnp.bfloat16).astype(jnp.float32)
    mid = (gate - big).astype(jnp.bfloat16).astype(jnp.float32)
    low = (gate - big) - mid
    for e in range(owned):
        here = lane == pos_ref[0, e:e + 1, :]
        rows = slice(e * cap, (e + 1) * cap)
        for ref, part in ((big_ref, big), (mid_ref, mid), (low_ref, low)):
            ref[rows, :] = jnp.where(here, part[e:e + 1, :], 0.0).astype(jnp.bfloat16)
    width = 512
    over = (((0,), (0,)), ((), ()))
    for c in range(out_ref.shape[1] // width):
        cols = slice(c * width, (c + 1) * width)
        done = done_ref[:, :, 0, :, cols].reshape(owned * cap, width)
        total = lax.dot_general(low_ref[...], done, over, preferred_element_type=jnp.float32)
        total += lax.dot_general(mid_ref[...], done, over, preferred_element_type=jnp.float32)
        out_ref[:, cols] = total + lax.dot_general(big_ref[...], done, over, preferred_element_type=jnp.float32)


def combine(pos, gates, done):
    n, owned, toks = pos.shape
    parts, dim = done.shape[1], done.shape[4]
    table = pl.BlockSpec((1, owned, toks), lambda s: (s, 0, 0))
    return pl.pallas_call(
        combine_kernel,
        grid=(n,),
        in_specs=[table, table, pl.BlockSpec((owned, parts, 1, SLOT, dim), lambda s: (0, 0, s, 0, 0))],
        out_specs=pl.BlockSpec((toks, dim), lambda s: (s, 0)),
        out_shape=jax.ShapeDtypeStruct((n * toks, dim), jnp.float32),
        scratch_shapes=[pltpu.VMEM((owned * parts * SLOT, toks), jnp.bfloat16)] * 3,
        compiler_params=pltpu.CompilerParams(vmem_limit_bytes=60 * 2 ** 20),
        cost_estimate=pl.CostEstimate(flops=6 * n * owned * parts * SLOT * toks * dim, bytes_accessed=60_000_000, transcendentals=0),
        name="combine",
    )(pos, gates, done)


def solution(mesh):
    tok_spec = P(('dp', 'ep'))
    row_spec = P('ep')
    groups = mesh.shape['dp']
    n = mesh.shape['ep']

    def gather_rows(weight):
        rows = weight.shape[0]
        if rows % (8 * groups):
            return lax.all_gather(weight, 'ep', axis=0, tiled=True)
        share = rows // groups
        piece = lax.dynamic_slice_in_dim(weight, lax.axis_index('dp') * share, share, 0)
        return lax.all_gather(piece, ('ep', 'dp'), axis=0, tiled=True)

    def local_layer(tokens, w_query, w_key, w_value, w_out, w_router, w_one, w_three, w_two, expert_ids):
        seq_count, seq_len, model_dim = tokens.shape
        choices = expert_ids.shape[2]
        experts = w_router.shape[1]
        owned = w_one.shape[0]
        toks = seq_count * seq_len
        parts = 2 * toks * choices // experts // SLOT

        member, slots = slot_table(expert_ids.reshape(toks, choices), experts)
        pos = lax.all_to_all(slots.T.reshape(n, owned, toks), 'ep', 0, 0, tiled=True)
        need = jnp.max(pos, axis=(0, 2)) // SLOT + 1

        full_query = gather_rows(w_query)
        full_key = gather_rows(w_key)
        full_value = gather_rows(w_value)
        full_out = gather_rows(w_out)
        hidden = attention_layer(tokens, full_query, full_key, full_value, full_out).reshape(toks, model_dim)
        normed, gates_local = dense_gates(hidden, w_router, member)
        u_all = lax.all_gather(normed, 'ep', axis=0, tiled=True)
        gates = lax.all_to_all(gates_local.T.reshape(n, owned, toks), 'ep', 0, 0, tiled=True)
        rows = dispatch(pos, u_all, parts)
        done = ffn(need, rows, w_one, w_three, w_two)
        partial = combine(pos, gates, done)
        mixed = lax.psum_scatter(partial, 'ep', scatter_dimension=0, tiled=True)
        layer_out = (hidden.astype(jnp.float32) + mixed).astype(jnp.bfloat16)
        return layer_out.reshape(seq_count, seq_len, model_dim)

    return jax.shard_map(local_layer, mesh=mesh, in_specs=(tok_spec, row_spec, row_spec, row_spec, row_spec, P(), row_spec, row_spec, row_spec, tok_spec), out_specs=tok_spec, check_vma=False)
```

```python
import functools

import jax
import jax.numpy as jnp
from jax import lax
from jax.experimental import pallas as pl
from jax.experimental.pallas import tpu as pltpu
from jax.sharding import PartitionSpec as P

EPS = 1e-6
SLOT = 16
MESH = pl.DeviceIdType.MESH


def rms_norm(vals):
    wide = vals.astype(jnp.float32)
    return wide * lax.rsqrt(jnp.mean(wide * wide, axis=-1, keepdims=True) + EPS)


def attend_kernel(mesh_n, seq_len, x_ref, wq_ref, wk_ref, wv_ref, wo_ref, h_ref, fq_ref, fk_ref, fv_ref, fo_ref,
                  n_ref, q_ref, k_ref, v_ref, wide_ref, tall_ref, send, recv, load_sem):
    me = lax.axis_index('ep')
    dp = lax.axis_index('dp')
    core = me % 2
    odd = dp % 2
    right = (me + 2) % mesh_n
    left = (me + mesh_n - 2) % mesh_n
    across = (me + mesh_n // 2) % mesh_n
    sibling = me + 1 - 2 * core
    partner = dp + 1 - 2 * odd
    own_refs = (wq_ref, wk_ref, wv_ref, wo_ref)
    full_refs = (fq_ref, fk_ref, fv_ref, fo_ref)

    barrier = pltpu.get_barrier_semaphore()
    for peer in (right, left, sibling):
        pl.semaphore_signal(barrier, inc=1, device_id={'ep': peer}, device_id_type=MESH)
    pl.semaphore_signal(barrier, inc=1, device_id={'dp': partner}, device_id_type=MESH)
    pl.semaphore_wait(barrier, 4)

    def spans(m):
        unit = own_refs[m].shape[0] // 16
        def at(even_off, odd_off, size):
            return pl.ds(pl.multiple_of((even_off + odd * (odd_off - even_off)) * unit, unit), size * unit)
        return {'F': at(0, 10, 6), 'S': at(6, 5, 5), 'X': at(0, 5, 11), 'ZS': at(0, 11, 5), 'ZR': at(11, 0, 5)}

    def ways(m):
        return (right, left) if m % 2 == 0 else (left, right)

    def copy(m, slot, src, dst, peer):
        return pltpu.make_async_remote_copy(src_ref=src, dst_ref=dst, send_sem=send.at[m, slot], recv_sem=recv.at[m, slot],
                                            device_id=peer, device_id_type=MESH)

    def outgoing(m, slot):
        full, own, span, (fore, back) = full_refs[m], own_refs[m], spans(m), ways(m)
        if slot < 4:
            rows = span['FSSF'[slot]]
            return copy(m, slot, own.at[rows], full.at[me, rows], {'ep': fore if slot < 2 else back})
        if slot < 6:
            rows, source = (span['F'], back) if slot == 4 else (span['S'], fore)
            return copy(m, slot, full.at[source, rows], full.at[source, rows], {'ep': fore if slot == 4 else back})
        if slot < 9:
            source, rows = (back, fore, across)[slot - 6], span['ZS']
            return copy(m, slot, full.at[source, rows], full.at[source, rows], {'dp': partner})
        if slot == 9:
            return copy(m, slot, own, full.at[me], {'ep': sibling})
        source, rows = (back, fore, across)[(slot - 10) % 3], span['X' if slot < 13 else 'ZR']
        return copy(m, slot, full.at[source, rows], full.at[source, rows], {'ep': sibling})

    def arrived(m, slot):
        full, span, (fore, back) = full_refs[m], spans(m), ways(m)
        if slot < 4:
            dst = full.at[back if slot < 2 else fore, span['FSSF'[slot]]]
        elif slot < 6:
            dst = full.at[across, span['F' if slot == 4 else 'S']]
        elif slot < 9:
            dst = full.at[(back, fore, across)[slot - 6], span['ZR']]
        elif slot == 9:
            dst = full.at[sibling]
        else:
            source = (back, fore, across)[(slot - 10) % 3]
            dst = full.at[source + 1 - 2 * core, span['X' if slot < 13 else 'ZR']]
        copy(m, slot, dst, dst, {'ep': sibling}).wait_recv()

    def start(m, *slots):
        for slot in slots:
            outgoing(m, slot).start()

    def own(m):
        start(m, 0, 2, 1, 3, 9)

    def near(m):
        arrived(m, 0)
        start(m, 4, 6)
        arrived(m, 2)
        start(m, 5)
        arrived(m, 1)
        start(m, 10)
        arrived(m, 3)
        start(m, 7, 11)

    def far(m):
        arrived(m, 4)
        start(m, 8)
        arrived(m, 5)
        start(m, 12)

    def zside(m):
        for slot in (6, 7, 8):
            arrived(m, slot)
            start(m, slot + 7)

    def finish(m):
        for slot in range(9, 16):
            arrived(m, slot)

    def stream(m, buf, width, body):
        full, mine = full_refs[m], own_refs[m]
        total = full.shape[2] // width
        def cols(c):
            return pl.ds(pl.multiple_of(c * width, width), width)
        def fetch(c, slot):
            pltpu.make_async_copy(mine.at[:, cols(c)], buf.at[slot, me], load_sem.at[slot]).start()
            for j in range(1, mesh_n):
                owner = (me + j) % mesh_n
                pltpu.make_async_copy(full.at[owner, :, cols(c)], buf.at[slot, owner], load_sem.at[slot]).start()
        fetch(0, 0)
        def step(c, carry):
            slot = c % 2
            @pl.when(c + 1 < total)
            def _():
                fetch(c + 1, 1 - slot)
            pltpu.make_async_copy(full.at[:, :, cols(c)], buf.at[slot], load_sem.at[slot]).wait()
            body(cols(c), buf[slot].reshape(full.shape[0] * full.shape[1], width))
            return carry
        lax.fori_loop(0, total, step, 0)

    def project(m, out):
        def body(cols, chunk):
            out[:, cols] = jnp.dot(n_ref[...], chunk, preferred_element_type=jnp.float32).astype(jnp.bfloat16)
        stream(m, wide_ref, wide_ref.shape[3], body)

    head_dim = 128
    seqs = x_ref.shape[0] // seq_len
    causal = lax.broadcasted_iota(jnp.int32, (seq_len, seq_len), 0) >= lax.broadcasted_iota(jnp.int32, (seq_len, seq_len), 1)

    def attention(first, last):
        def step(i, carry):
            for b in range(seqs):
                rows = slice(b * seq_len, (b + 1) * seq_len)
                for j in range(2):
                    cols = pl.ds(pl.multiple_of((2 * i + j) * head_dim, head_dim), head_dim)
                    scores = lax.dot_general(q_ref[rows, cols], k_ref[rows, cols], (((1,), (1,)), ((), ())),
                                             preferred_element_type=jnp.float32) * head_dim ** -0.5
                    scores = jnp.where(causal, scores, -jnp.inf)
                    grown = jnp.exp(scores - jnp.max(scores, axis=1, keepdims=True))
                    weights = (grown * (1.0 / jnp.sum(grown, axis=1, keepdims=True))).astype(jnp.bfloat16)
                    q_ref[rows, cols] = jnp.dot(weights, v_ref[rows, cols], preferred_element_type=jnp.float32).astype(jnp.bfloat16)
            return carry
        lax.fori_loop(first, last, step, 0)

    own(0)
    own(1)
    wide = x_ref[...].astype(jnp.float32)
    n_ref[...] = (wide * lax.rsqrt(jnp.mean(wide * wide, axis=-1, keepdims=True) + EPS)).astype(jnp.bfloat16)
    near(0)
    own(2)
    near(1)
    far(0)
    zside(0)
    finish(0)
    project(0, q_ref)
    near(2)
    far(1)
    zside(1)
    finish(1)
    own(3)
    project(1, k_ref)
    far(2)
    zside(2)
    finish(2)
    project(2, v_ref)
    pairs = q_ref.shape[1] // head_dim // 2
    attention(0, pairs // 2)
    near(3)
    attention(pairs // 2, pairs)
    far(3)
    zside(3)
    finish(3)

    def out_body(cols, chunk):
        mixed = jnp.dot(q_ref[...], chunk, preferred_element_type=jnp.float32)
        h_ref[:, cols] = (x_ref[:, cols].astype(jnp.float32) + mixed).astype(jnp.bfloat16)
    stream(3, tall_ref, tall_ref.shape[3], out_body)
    for m in range(4):
        for slot in range(16):
            outgoing(m, slot).wait_send()


def attend(mesh_n, seq_len, x, wq, wk, wv, wo):
    toks, dim = x.shape
    width = wq.shape[1]
    bf = jnp.bfloat16
    vmem = pl.BlockSpec(memory_space=pltpu.VMEM)
    hbm = pl.BlockSpec(memory_space=pltpu.HBM)
    fulls = [jax.ShapeDtypeStruct((mesh_n,) + w.shape, bf) for w in (wq, wk, wv, wo)]
    out = pl.pallas_call(
        functools.partial(attend_kernel, mesh_n, seq_len),
        in_specs=[vmem, hbm, hbm, hbm, hbm],
        out_specs=[vmem, hbm, hbm, hbm, hbm],
        out_shape=[jax.ShapeDtypeStruct((toks, dim), bf)] + fulls,
        scratch_shapes=[
            pltpu.VMEM((toks, dim), bf),
            pltpu.VMEM((toks, width), bf),
            pltpu.VMEM((toks, width), bf),
            pltpu.VMEM((toks, width), bf),
            pltpu.VMEM((2, mesh_n, wq.shape[0], min(512, width)), bf),
            pltpu.VMEM((2, mesh_n, wo.shape[0], min(256, dim)), bf),
            pltpu.SemaphoreType.DMA((4, 16)),
            pltpu.SemaphoreType.DMA((4, 16)),
            pltpu.SemaphoreType.DMA((2,)),
        ],
        compiler_params=pltpu.CompilerParams(collective_id=0, has_side_effects=True, vmem_limit_bytes=56 * 2 ** 20),
        cost_estimate=pl.CostEstimate(flops=8 * toks * dim * width, bytes_accessed=200_000_000, transcendentals=0),
        name='attend',
    )(x, wq, wk, wv, wo)
    return out[0]


def slot_table(ids_flat, experts):
    tok_count = ids_flat.shape[0]
    member = jnp.any(ids_flat[:, :, None] == jnp.arange(experts, dtype=jnp.int32), axis=1)
    strict = lax.broadcasted_iota(jnp.int32, (tok_count, tok_count), 0) > lax.broadcasted_iota(jnp.int32, (tok_count, tok_count), 1)
    before = jnp.dot(strict.astype(jnp.bfloat16), member.astype(jnp.bfloat16), preferred_element_type=jnp.float32)
    return member, jnp.where(member, before.astype(jnp.int32), -1)


def dense_gates(hidden, w_router, member):
    normed = rms_norm(hidden)
    logits = jnp.dot(normed, w_router, precision=lax.Precision.HIGHEST, preferred_element_type=jnp.float32)
    top = jnp.max(jnp.where(member, logits, -jnp.inf), axis=1, keepdims=True)
    grown = jnp.where(member, jnp.exp(jnp.where(member, logits, top) - top), 0.0)
    return normed.astype(jnp.bfloat16), grown / jnp.sum(grown, axis=1, keepdims=True)


def dispatch_kernel(pos_ref, u_ref, out_ref, hot_ref):
    owned, toks = pos_ref.shape[1], pos_ref.shape[2]
    parts = out_ref.shape[1]
    cap = parts * SLOT
    lane = lax.broadcasted_iota(jnp.int32, (cap, toks), 0)
    for e in range(owned):
        hot_ref[e * cap:(e + 1) * cap, :] = jnp.where(lane == pos_ref[0, e:e + 1, :], 1.0, 0.0).astype(jnp.bfloat16)
    width = 512
    for c in range(u_ref.shape[1] // width):
        cols = slice(c * width, (c + 1) * width)
        rows = jnp.dot(hot_ref[...], u_ref[:, cols], preferred_element_type=jnp.float32).astype(jnp.bfloat16)
        out_ref[:, :, 0, :, cols] = rows.reshape(owned, parts, SLOT, width)


def dispatch(pos, u_all, parts):
    n, owned, toks = pos.shape
    dim = u_all.shape[1]
    return pl.pallas_call(
        dispatch_kernel,
        grid=(n,),
        in_specs=[pl.BlockSpec((1, owned, toks), lambda s: (s, 0, 0)), pl.BlockSpec((toks, dim), lambda s: (s, 0))],
        out_specs=pl.BlockSpec((owned, parts, 1, SLOT, dim), lambda s: (0, 0, s, 0, 0)),
        out_shape=jax.ShapeDtypeStruct((owned, parts, n, SLOT, dim), jnp.bfloat16),
        scratch_shapes=[pltpu.VMEM((owned * parts * SLOT, toks), jnp.bfloat16)],
        compiler_params=pltpu.CompilerParams(vmem_limit_bytes=60 * 2 ** 20),
        cost_estimate=pl.CostEstimate(flops=2 * n * owned * parts * SLOT * toks * dim, bytes_accessed=40_000_000, transcendentals=0),
        name="dispatch",
    )(pos, u_all)


def ffn_kernel(need_ref, rows_ref, one_ref, three_ref, two_ref, out_ref):
    parts, n = rows_ref.shape[1], rows_ref.shape[2]
    dim = rows_ref.shape[4]
    step = n * SLOT
    need = need_ref[pl.program_id(0)]
    for used in range(parts + 1):
        @pl.when(need == used)
        def _():
            if used:
                rows = rows_ref[0, :used].reshape(used * step, dim)
                first = jnp.dot(rows, one_ref[0], preferred_element_type=jnp.float32)
                third = jnp.dot(rows, three_ref[0], preferred_element_type=jnp.float32)
                acted = (jax.nn.silu(first) * third).astype(jnp.bfloat16)
                done = jnp.dot(acted, two_ref[0], preferred_element_type=jnp.float32).astype(jnp.bfloat16)
                out_ref[0, :used] = done.reshape(used, n, SLOT, dim)
            if used < parts:
                out_ref[0, used:] = jnp.zeros((parts - used, n, SLOT, dim), jnp.bfloat16)


def ffn(need, rows, w_one, w_three, w_two):
    owned, parts, n, _, dim = rows.shape
    inner = w_one.shape[2]
    tile = pl.BlockSpec((1, parts, n, SLOT, dim), lambda e, _: (e, 0, 0, 0, 0))
    return pl.pallas_call(
        ffn_kernel,
        grid_spec=pltpu.PrefetchScalarGridSpec(
            num_scalar_prefetch=1,
            grid=(owned,),
            in_specs=[
                tile,
                pl.BlockSpec((1, dim, inner), lambda e, _: (e, 0, 0)),
                pl.BlockSpec((1, dim, inner), lambda e, _: (e, 0, 0)),
                pl.BlockSpec((1, inner, dim), lambda e, _: (e, 0, 0)),
            ],
            out_specs=tile,
        ),
        out_shape=jax.ShapeDtypeStruct(rows.shape, jnp.bfloat16),
        compiler_params=pltpu.CompilerParams(vmem_limit_bytes=60 * 2 ** 20),
        cost_estimate=pl.CostEstimate(flops=6 * rows.size * inner, bytes_accessed=200_000_000, transcendentals=0),
        name="ffn",
    )(need, rows, w_one, w_three, w_two)


def combine_kernel(pos_ref, gate_ref, done_ref, out_ref, big_ref, mid_ref, low_ref):
    owned, toks = pos_ref.shape[1], pos_ref.shape[2]
    parts = done_ref.shape[1]
    cap = parts * SLOT
    lane = lax.broadcasted_iota(jnp.int32, (cap, toks), 0)
    gate = gate_ref[0]
    big = gate.astype(jnp.bfloat16).astype(jnp.float32)
    mid = (gate - big).astype(jnp.bfloat16).astype(jnp.float32)
    low = (gate - big) - mid
    for e in range(owned):
        here = lane == pos_ref[0, e:e + 1, :]
        rows = slice(e * cap, (e + 1) * cap)
        for ref, part in ((big_ref, big), (mid_ref, mid), (low_ref, low)):
            ref[rows, :] = jnp.where(here, part[e:e + 1, :], 0.0).astype(jnp.bfloat16)
    width = 512
    over = (((0,), (0,)), ((), ()))
    for c in range(out_ref.shape[1] // width):
        cols = slice(c * width, (c + 1) * width)
        done = done_ref[:, :, 0, :, cols].reshape(owned * cap, width)
        total = lax.dot_general(low_ref[...], done, over, preferred_element_type=jnp.float32)
        total += lax.dot_general(mid_ref[...], done, over, preferred_element_type=jnp.float32)
        out_ref[:, cols] = total + lax.dot_general(big_ref[...], done, over, preferred_element_type=jnp.float32)


def combine(pos, gates, done):
    n, owned, toks = pos.shape
    parts, dim = done.shape[1], done.shape[4]
    table = pl.BlockSpec((1, owned, toks), lambda s: (s, 0, 0))
    return pl.pallas_call(
        combine_kernel,
        grid=(n,),
        in_specs=[table, table, pl.BlockSpec((owned, parts, 1, SLOT, dim), lambda s: (0, 0, s, 0, 0))],
        out_specs=pl.BlockSpec((toks, dim), lambda s: (s, 0)),
        out_shape=jax.ShapeDtypeStruct((n * toks, dim), jnp.float32),
        scratch_shapes=[pltpu.VMEM((owned * parts * SLOT, toks), jnp.bfloat16)] * 3,
        compiler_params=pltpu.CompilerParams(vmem_limit_bytes=60 * 2 ** 20),
        cost_estimate=pl.CostEstimate(flops=6 * n * owned * parts * SLOT * toks * dim, bytes_accessed=60_000_000, transcendentals=0),
        name="combine",
    )(pos, gates, done)


def solution(mesh):
    tok_spec = P(('dp', 'ep'))
    row_spec = P('ep')
    n = mesh.shape['ep']

    def local_layer(tokens, w_query, w_key, w_value, w_out, w_router, w_one, w_three, w_two, expert_ids):
        seq_count, seq_len, model_dim = tokens.shape
        choices = expert_ids.shape[2]
        experts = w_router.shape[1]
        owned = w_one.shape[0]
        toks = seq_count * seq_len
        parts = 2 * toks * choices // experts // SLOT

        member, slots = slot_table(expert_ids.reshape(toks, choices), experts)
        pos = lax.all_to_all(slots.T.reshape(n, owned, toks), 'ep', 0, 0, tiled=True)
        need = jnp.max(pos, axis=(0, 2)) // SLOT + 1

        flat = [w.reshape(w.shape[0], -1) for w in (w_query, w_key, w_value, w_out)]
        hidden = attend(n, seq_len, tokens.reshape(toks, model_dim), *flat)
        normed, gates_local = dense_gates(hidden, w_router, member)
        u_all = lax.all_gather(normed, 'ep', axis=0, tiled=True)
        gates = lax.all_to_all(gates_local.T.reshape(n, owned, toks), 'ep', 0, 0, tiled=True)
        rows = dispatch(pos, u_all, parts)
        done = ffn(need, rows, w_one, w_three, w_two)
        partial = combine(pos, gates, done)
        mixed = lax.psum_scatter(partial, 'ep', scatter_dimension=0, tiled=True)
        layer_out = (hidden.astype(jnp.float32) + mixed).astype(jnp.bfloat16)
        return layer_out.reshape(seq_count, seq_len, model_dim)

    return jax.shard_map(local_layer, mesh=mesh, in_specs=(tok_spec, row_spec, row_spec, row_spec, row_spec, P(), row_spec, row_spec, row_spec, tok_spec), out_specs=tok_spec, check_vma=False)
```

```python
import functools

import jax
import jax.numpy as jnp
from jax import lax
from jax.experimental import pallas as pl
from jax.experimental.pallas import tpu as pltpu
from jax.sharding import PartitionSpec as P

EPS = 1e-6
SLOT = 16
MESH = pl.DeviceIdType.MESH


def rms_norm(vals):
    wide = vals.astype(jnp.float32)
    return wide * lax.rsqrt(jnp.mean(wide * wide, axis=-1, keepdims=True) + EPS)


def attend_kernel(mesh_n, seq_len, x_ref, wq_ref, wk_ref, wv_ref, wo_ref, h_ref, fq_ref, fk_ref, fv_ref, fo_ref,
                  n_ref, q_ref, k_ref, v_ref, wide_ref, tall_ref, sum_ref, send, recv, load_sem):
    me = lax.axis_index('ep')
    dp = lax.axis_index('dp')
    core = me % 2
    odd = dp % 2
    right = (me + 2) % mesh_n
    left = (me + mesh_n - 2) % mesh_n
    across = (me + mesh_n // 2) % mesh_n
    sibling = me + 1 - 2 * core
    partner = dp + 1 - 2 * odd
    own_refs = (wq_ref, wk_ref, wv_ref, wo_ref)
    full_refs = (fq_ref, fk_ref, fv_ref, fo_ref)

    barrier = pltpu.get_barrier_semaphore()
    for peer in (right, left, sibling):
        pl.semaphore_signal(barrier, inc=1, device_id={'ep': peer}, device_id_type=MESH)
    pl.semaphore_signal(barrier, inc=1, device_id={'dp': partner}, device_id_type=MESH)
    pl.semaphore_wait(barrier, 4)

    def spans(m):
        unit = own_refs[m].shape[0] // 16
        def at(even_off, odd_off, size):
            return pl.ds(pl.multiple_of((even_off + odd * (odd_off - even_off)) * unit, unit), size * unit)
        return {'F': at(0, 10, 6), 'S': at(6, 5, 5), 'X': at(0, 5, 11), 'ZS': at(0, 11, 5), 'ZR': at(11, 0, 5)}

    def ways(m):
        return (right, left) if m % 2 == 0 else (left, right)

    def copy(m, slot, src, dst, peer):
        return pltpu.make_async_remote_copy(src_ref=src, dst_ref=dst, send_sem=send.at[m, slot], recv_sem=recv.at[m, slot],
                                            device_id=peer, device_id_type=MESH)

    def outgoing(m, slot):
        full, own, span, (fore, back) = full_refs[m], own_refs[m], spans(m), ways(m)
        if slot < 4:
            rows = span['FSSF'[slot]]
            return copy(m, slot, own.at[rows], full.at[me, rows], {'ep': fore if slot < 2 else back})
        if slot < 6:
            rows, source = (span['F'], back) if slot == 4 else (span['S'], fore)
            return copy(m, slot, full.at[source, rows], full.at[source, rows], {'ep': fore if slot == 4 else back})
        if slot < 9:
            source, rows = (back, fore, across)[slot - 6], span['ZS']
            return copy(m, slot, full.at[source, rows], full.at[source, rows], {'dp': partner})
        if slot == 9:
            return copy(m, slot, own, full.at[me], {'ep': sibling})
        source, rows = (back, fore, across)[(slot - 10) % 3], span['X' if slot < 13 else 'ZR']
        return copy(m, slot, full.at[source, rows], full.at[source, rows], {'ep': sibling})

    def arrived(m, slot):
        full, span, (fore, back) = full_refs[m], spans(m), ways(m)
        if slot < 4:
            dst = full.at[back if slot < 2 else fore, span['FSSF'[slot]]]
        elif slot < 6:
            dst = full.at[across, span['F' if slot == 4 else 'S']]
        elif slot < 9:
            dst = full.at[(back, fore, across)[slot - 6], span['ZR']]
        elif slot == 9:
            dst = full.at[sibling]
        else:
            source = (back, fore, across)[(slot - 10) % 3]
            dst = full.at[source + 1 - 2 * core, span['X' if slot < 13 else 'ZR']]
        copy(m, slot, dst, dst, {'ep': sibling}).wait_recv()

    def start(m, *slots):
        for slot in slots:
            outgoing(m, slot).start()

    def own(m):
        start(m, 0, 2, 1, 3, 9)

    def near_first(m):
        arrived(m, 0)
        start(m, 4, 6)
        arrived(m, 2)
        start(m, 5)

    def near_last(m):
        arrived(m, 1)
        start(m, 10)
        arrived(m, 3)
        start(m, 7, 11)

    def near(m):
        near_first(m)
        near_last(m)

    def far(m):
        arrived(m, 4)
        start(m, 8)
        arrived(m, 5)
        start(m, 12)

    def zside(m, slots=(6, 7, 8)):
        for slot in slots:
            arrived(m, slot)
            start(m, slot + 7)

    def finish(m, slots=tuple(range(9, 16))):
        for slot in slots:
            arrived(m, slot)

    def stream(m, buf, width, body):
        full, mine = full_refs[m], own_refs[m]
        total = full.shape[2] // width
        def cols(c):
            return pl.ds(pl.multiple_of(c * width, width), width)
        def fetch(c, slot):
            pltpu.make_async_copy(mine.at[:, cols(c)], buf.at[slot, me], load_sem.at[slot]).start()
            for j in range(1, mesh_n):
                owner = (me + j) % mesh_n
                pltpu.make_async_copy(full.at[owner, :, cols(c)], buf.at[slot, owner], load_sem.at[slot]).start()
        fetch(0, 0)
        def step(c, carry):
            slot = c % 2
            @pl.when(c + 1 < total)
            def _():
                fetch(c + 1, 1 - slot)
            pltpu.make_async_copy(full.at[:, :, cols(c)], buf.at[slot], load_sem.at[slot]).wait()
            body(cols(c), buf[slot].reshape(full.shape[0] * full.shape[1], width))
            return carry
        lax.fori_loop(0, total, step, 0)

    def project(m, out):
        def body(cols, chunk):
            out[:, cols] = jnp.dot(n_ref[...], chunk, preferred_element_type=jnp.float32).astype(jnp.bfloat16)
        stream(m, wide_ref, wide_ref.shape[3], body)

    head_dim = 128
    seqs = x_ref.shape[0] // seq_len
    causal = lax.broadcasted_iota(jnp.int32, (seq_len, seq_len), 0) >= lax.broadcasted_iota(jnp.int32, (seq_len, seq_len), 1)

    def attention(first, last):
        def step(i, carry):
            for b in range(seqs):
                rows = slice(b * seq_len, (b + 1) * seq_len)
                for j in range(2):
                    cols = pl.ds(pl.multiple_of((2 * i + j) * head_dim, head_dim), head_dim)
                    scores = lax.dot_general(q_ref[rows, cols], k_ref[rows, cols], (((1,), (1,)), ((), ())),
                                             preferred_element_type=jnp.float32) * head_dim ** -0.5
                    scores = jnp.where(causal, scores, -jnp.inf)
                    grown = jnp.exp(scores - jnp.max(scores, axis=1, keepdims=True))
                    weights = (grown * (1.0 / jnp.sum(grown, axis=1, keepdims=True))).astype(jnp.bfloat16)
                    q_ref[rows, cols] = jnp.dot(weights, v_ref[rows, cols], preferred_element_type=jnp.float32).astype(jnp.bfloat16)
            return carry
        lax.fori_loop(first, last, step, 0)

    own(0)
    own(1)
    wide = x_ref[...].astype(jnp.float32)
    n_ref[...] = (wide * lax.rsqrt(jnp.mean(wide * wide, axis=-1, keepdims=True) + EPS)).astype(jnp.bfloat16)
    near(0)
    own(2)
    near(1)
    far(0)
    zside(0)
    finish(0)
    project(0, q_ref)
    near(2)
    own(3)
    far(1)
    zside(1)
    finish(1)
    project(1, k_ref)
    far(2)
    zside(2)
    finish(2)
    near_first(3)
    project(2, v_ref)
    pairs = q_ref.shape[1] // head_dim // 2
    attention(0, pairs // 2)
    near_last(3)
    attention(pairs // 2, pairs)
    zside(3, (6, 7))
    finish(3, (9, 10, 11, 13, 14))

    fore, back = ways(3)
    def twin(source):
        return source + 1 - 2 * core
    depth = fo_ref.shape[1]
    order = (me, sibling, back, fore, twin(back), twin(fore), across, twin(across))
    def fetch(i):
        source = wo_ref if i == 0 else fo_ref.at[order[i]]
        pltpu.make_async_copy(source, tall_ref.at[i % 2], load_sem.at[i % 2]).start()
    def gather_product(first, last):
        fetch(first)
        for i in range(first, last):
            if i + 1 < last:
                fetch(i + 1)
            pltpu.make_async_copy(fo_ref.at[order[i]], tall_ref.at[i % 2], load_sem.at[i % 2]).wait()
            heads = pl.ds(pl.multiple_of(order[i] * depth, depth), depth)
            width = min(512, sum_ref.shape[1])
            def part(c, carry):
                cols = pl.ds(pl.multiple_of(c * width, width), width)
                product = jnp.dot(q_ref[:, heads], tall_ref[i % 2, :, cols], preferred_element_type=jnp.float32)
                if i == 0:
                    sum_ref[:, cols] = x_ref[:, cols].astype(jnp.float32) + product
                elif i < mesh_n - 1:
                    sum_ref[:, cols] += product
                else:
                    h_ref[:, cols] = (sum_ref[:, cols] + product).astype(jnp.bfloat16)
                return carry
            lax.fori_loop(0, sum_ref.shape[1] // width, part, 0)
    gather_product(0, mesh_n - 2)
    far(3)
    zside(3, (8,))
    finish(3, (12, 15))
    gather_product(mesh_n - 2, mesh_n)
    for m in range(4):
        for slot in range(16):
            outgoing(m, slot).wait_send()


def attend(mesh_n, seq_len, x, wq, wk, wv, wo):
    toks, dim = x.shape
    width = wq.shape[1]
    bf = jnp.bfloat16
    vmem = pl.BlockSpec(memory_space=pltpu.VMEM)
    hbm = pl.BlockSpec(memory_space=pltpu.HBM)
    fulls = [jax.ShapeDtypeStruct((mesh_n,) + w.shape, bf) for w in (wq, wk, wv, wo)]
    out = pl.pallas_call(
        functools.partial(attend_kernel, mesh_n, seq_len),
        in_specs=[vmem, hbm, hbm, hbm, hbm],
        out_specs=[vmem, hbm, hbm, hbm, hbm],
        out_shape=[jax.ShapeDtypeStruct((toks, dim), bf)] + fulls,
        scratch_shapes=[
            pltpu.VMEM((toks, dim), bf),
            pltpu.VMEM((toks, width), bf),
            pltpu.VMEM((toks, width), bf),
            pltpu.VMEM((toks, width), bf),
            pltpu.VMEM((2, mesh_n, wq.shape[0], min(512, width)), bf),
            pltpu.VMEM((2,) + wo.shape, bf),
            pltpu.VMEM((toks, dim), jnp.float32),
            pltpu.SemaphoreType.DMA((4, 16)),
            pltpu.SemaphoreType.DMA((4, 16)),
            pltpu.SemaphoreType.DMA((2,)),
        ],
        compiler_params=pltpu.CompilerParams(collective_id=0, has_side_effects=True, vmem_limit_bytes=56 * 2 ** 20),
        cost_estimate=pl.CostEstimate(flops=8 * toks * dim * width, bytes_accessed=200_000_000, transcendentals=0),
        name='attend',
    )(x, wq, wk, wv, wo)
    return out[0]


def slot_table(ids_flat, experts):
    tok_count = ids_flat.shape[0]
    member = jnp.any(ids_flat[:, :, None] == jnp.arange(experts, dtype=jnp.int32), axis=1)
    strict = lax.broadcasted_iota(jnp.int32, (tok_count, tok_count), 0) > lax.broadcasted_iota(jnp.int32, (tok_count, tok_count), 1)
    before = jnp.dot(strict.astype(jnp.bfloat16), member.astype(jnp.bfloat16), preferred_element_type=jnp.float32)
    return member, jnp.where(member, before.astype(jnp.int32), -1)


def dense_gates(hidden, w_router, member):
    normed = rms_norm(hidden)
    logits = jnp.dot(normed, w_router, precision=lax.Precision.HIGHEST, preferred_element_type=jnp.float32)
    top = jnp.max(jnp.where(member, logits, -jnp.inf), axis=1, keepdims=True)
    grown = jnp.where(member, jnp.exp(jnp.where(member, logits, top) - top), 0.0)
    return normed.astype(jnp.bfloat16), grown / jnp.sum(grown, axis=1, keepdims=True)


def neighbours(mesh_n):
    me = lax.axis_index('ep')
    core = me % 2
    sibling = me + 1 - 2 * core
    return me, core, sibling, (me + 2) % mesh_n, (me + mesh_n - 2) % mesh_n, (me + mesh_n // 2) % mesh_n


def meet(mesh_n, me):
    barrier = pltpu.get_barrier_semaphore()
    for j in range(1, mesh_n):
        pl.semaphore_signal(barrier, inc=1, device_id={'ep': (me + j) % mesh_n}, device_id_type=MESH)
    pl.semaphore_wait(barrier, mesh_n - 1)


def route_kernel(mesh_n, u_ref, mine_ref, rows_ref, tab_ref, all_ref, hot_ref, stage_ref, send, recv, tab_send, tab_recv, out_sem):
    me, core, sibling, right, left, across = neighbours(mesh_n)
    meet(mesh_n, me)
    toks = u_ref.shape[0]
    half = toks // 2
    lows, highs = pl.ds(0, half), pl.ds(half, half)

    def copy(slot, src, dst, peer):
        return pltpu.make_async_remote_copy(src_ref=src, dst_ref=dst, send_sem=send.at[slot], recv_sem=recv.at[slot],
                                            device_id={'ep': peer}, device_id_type=MESH)

    def outgoing(slot):
        if slot < 4:
            rows = (lows, highs, highs, lows)[slot]
            return copy(slot, u_ref.at[rows], all_ref.at[me, rows], right if slot < 2 else left)
        if slot == 4:
            return copy(slot, all_ref.at[left, lows], all_ref.at[left, lows], right)
        if slot == 5:
            return copy(slot, all_ref.at[right, highs], all_ref.at[right, highs], left)
        if slot == 6:
            return copy(slot, u_ref, all_ref.at[me], sibling)
        if slot < 9:
            source = left if slot == 7 else right
            return copy(slot, all_ref.at[source], all_ref.at[source], sibling)
        rows = lows if slot == 9 else highs
        return copy(slot, all_ref.at[across, rows], all_ref.at[across, rows], sibling)

    def arrived(*slots):
        for slot in slots:
            if slot < 4:
                dst = all_ref.at[left if slot < 2 else right, (lows, highs, highs, lows)[slot]]
            elif slot < 6:
                dst = all_ref.at[across, lows if slot == 4 else highs]
            elif slot == 6:
                dst = all_ref.at[sibling]
            elif slot < 9:
                dst = all_ref.at[(left if slot == 7 else right) + 1 - 2 * core]
            else:
                dst = all_ref.at[across + 1 - 2 * core, lows if slot == 9 else highs]
            copy(slot, dst, dst, sibling).wait_recv()

    def table(j, src, dst, peer):
        return pltpu.make_async_remote_copy(src_ref=src, dst_ref=dst, send_sem=tab_send.at[j], recv_sem=tab_recv.at[j],
                                            device_id={'ep': peer}, device_id_type=MESH)

    def table_out(j):
        peer = (me + j) % mesh_n
        return table(j, mine_ref.at[peer], tab_ref.at[me], peer)

    for j in range(1, mesh_n):
        table_out(j).start()
    for slot in (0, 2, 1, 3, 6):
        outgoing(slot).start()
    tab_ref[pl.ds(me, 1)] = mine_ref[pl.ds(me, 1)]
    for j in range(1, mesh_n):
        source = (me + mesh_n - j) % mesh_n
        table(j, tab_ref.at[source], tab_ref.at[source], source).wait_recv()

    owned = tab_ref.shape[1] // 2
    parts = rows_ref.shape[1]
    cap = parts * SLOT
    dim = u_ref.shape[1]
    width = min(512, dim)
    lane = lax.broadcasted_iota(jnp.int32, (cap, toks), 0).astype(jnp.float32)

    def flush(k, s):
        return pltpu.make_async_copy(stage_ref.at[k % 2], rows_ref.at[:, :, s], out_sem.at[k % 2])

    def send_rows(k, s, own=False):
        pos = tab_ref[pl.ds(s, 1), :owned][0]
        for e in range(owned):
            hot_ref[e * cap:(e + 1) * cap, :] = jnp.where(lane == pos[e:e + 1, :], 1.0, 0.0).astype(jnp.bfloat16)
        if k >= 2:
            flush(k, s).wait()
        def part(c, carry):
            cols = pl.ds(pl.multiple_of(c * width, width), width)
            block = u_ref[:, cols] if own else all_ref[pl.ds(s, 1), :, cols][0]
            rows = jnp.dot(hot_ref[...], block, preferred_element_type=jnp.float32).astype(jnp.bfloat16)
            stage_ref[k % 2, :, :, :, cols] = rows.reshape(owned, parts, SLOT, width)
            return carry
        lax.fori_loop(0, dim // width, part, 0)
        flush(k, s).start()

    send_rows(0, me, True)
    arrived(6)
    send_rows(1, sibling)
    arrived(0)
    outgoing(4).start()
    arrived(2)
    outgoing(5).start()
    arrived(1)
    outgoing(7).start()
    arrived(3)
    outgoing(8).start()
    send_rows(2, left)
    send_rows(3, right)
    arrived(7)
    send_rows(4, left + 1 - 2 * core)
    arrived(8)
    send_rows(5, right + 1 - 2 * core)
    arrived(4)
    outgoing(9).start()
    arrived(5)
    outgoing(10).start()
    send_rows(6, across)
    arrived(9, 10)
    send_rows(7, across + 1 - 2 * core)
    flush(6, me).wait()
    flush(7, me).wait()
    for j in range(1, mesh_n):
        table_out(j).wait_send()
    for slot in range(11):
        outgoing(slot).wait_send()


def route(mesh_n, u, table, parts):
    toks, dim = u.shape
    owned = table.shape[1] // 2
    bf = jnp.bfloat16
    vmem = pl.BlockSpec(memory_space=pltpu.VMEM)
    return pl.pallas_call(
        functools.partial(route_kernel, mesh_n),
        in_specs=[vmem, vmem],
        out_specs=[pl.BlockSpec(memory_space=pltpu.HBM), vmem],
        out_shape=[jax.ShapeDtypeStruct((owned, parts, mesh_n, SLOT, dim), bf), jax.ShapeDtypeStruct(table.shape, jnp.float32)],
        scratch_shapes=[
            pltpu.VMEM((mesh_n, toks, dim), bf),
            pltpu.VMEM((owned * parts * SLOT, toks), bf),
            pltpu.VMEM((2, owned, parts, SLOT, dim), bf),
            pltpu.SemaphoreType.DMA((11,)),
            pltpu.SemaphoreType.DMA((11,)),
            pltpu.SemaphoreType.DMA((mesh_n,)),
            pltpu.SemaphoreType.DMA((mesh_n,)),
            pltpu.SemaphoreType.DMA((2,)),
        ],
        compiler_params=pltpu.CompilerParams(collective_id=1, has_side_effects=True, vmem_limit_bytes=56 * 2 ** 20),
        cost_estimate=pl.CostEstimate(flops=2 * mesh_n * owned * parts * SLOT * toks * dim, bytes_accessed=40_000_000, transcendentals=0),
        name='route',
    )(u, table)


def ffn_kernel(need_ref, rows_ref, one_ref, three_ref, two_ref, out_ref):
    parts, n = rows_ref.shape[1], rows_ref.shape[2]
    dim = rows_ref.shape[4]
    step = n * SLOT
    need = need_ref[pl.program_id(0)]
    for used in range(parts + 1):
        @pl.when(need == used)
        def _():
            if used:
                rows = rows_ref[0, :used].reshape(used * step, dim)
                first = jnp.dot(rows, one_ref[0], preferred_element_type=jnp.float32)
                third = jnp.dot(rows, three_ref[0], preferred_element_type=jnp.float32)
                acted = (jax.nn.silu(first) * third).astype(jnp.bfloat16)
                done = jnp.dot(acted, two_ref[0], preferred_element_type=jnp.float32).astype(jnp.bfloat16)
                out_ref[0, :used] = done.reshape(used, n, SLOT, dim)
            if used < parts:
                out_ref[0, used:] = jnp.zeros((parts - used, n, SLOT, dim), jnp.bfloat16)


def ffn(need, rows, w_one, w_three, w_two):
    owned, parts, n, _, dim = rows.shape
    inner = w_one.shape[2]
    tile = pl.BlockSpec((1, parts, n, SLOT, dim), lambda e, _: (e, 0, 0, 0, 0))
    return pl.pallas_call(
        ffn_kernel,
        grid_spec=pltpu.PrefetchScalarGridSpec(
            num_scalar_prefetch=1,
            grid=(owned,),
            in_specs=[
                tile,
                pl.BlockSpec((1, dim, inner), lambda e, _: (e, 0, 0)),
                pl.BlockSpec((1, dim, inner), lambda e, _: (e, 0, 0)),
                pl.BlockSpec((1, inner, dim), lambda e, _: (e, 0, 0)),
            ],
            out_specs=tile,
        ),
        out_shape=jax.ShapeDtypeStruct(rows.shape, jnp.bfloat16),
        compiler_params=pltpu.CompilerParams(vmem_limit_bytes=60 * 2 ** 20),
        cost_estimate=pl.CostEstimate(flops=6 * rows.size * inner, bytes_accessed=200_000_000, transcendentals=0),
        name="ffn",
    )(need, rows, w_one, w_three, w_two)


def settle_kernel(mesh_n, tab_ref, h_ref, done_ref, y_ref, big_ref, mid_ref, low_ref, load_ref, pass_ref, twin_ref, sum_ref, far_ref, near_ref,
                  load_sem, twin_send, twin_recv, send, recv):
    me, core, sibling, right, left, across = neighbours(mesh_n)
    meet(mesh_n, me)
    toks, dim = h_ref.shape
    half = toks // 2
    lows, highs = slice(0, half), slice(half, toks)
    owned = tab_ref.shape[1] // 2
    parts = done_ref.shape[1]
    cap = parts * SLOT
    width = min(512, dim)
    lane = lax.broadcasted_iota(jnp.int32, (cap, toks), 0).astype(jnp.float32)
    over = (((0,), (0,)), ((), ()))
    chips = (across, right, left, me)
    jobs = [dest for chip in chips for dest in (chip + 1 - 2 * core, chip)]

    def fetch(k):
        return pltpu.make_async_copy(done_ref.at[:, :, jobs[k]], load_ref.at[k % 2], load_sem.at[k % 2])

    def partial(k, out, index):
        tab = tab_ref[pl.ds(jobs[k], 1)][0]
        pos, gate = tab[:owned], tab[owned:]
        big = gate.astype(jnp.bfloat16).astype(jnp.float32)
        mid = (gate - big).astype(jnp.bfloat16).astype(jnp.float32)
        low = (gate - big) - mid
        for e in range(owned):
            here = lane == pos[e:e + 1, :]
            for ref, piece in ((big_ref, big), (mid_ref, mid), (low_ref, low)):
                ref[e * cap:(e + 1) * cap, :] = jnp.where(here, piece[e:e + 1, :], 0.0).astype(jnp.bfloat16)
        fetch(k).wait()
        if k + 1 < len(jobs):
            fetch(k + 1).start()
        def part(c, carry):
            cols = pl.ds(pl.multiple_of(c * width, width), width)
            block = load_ref[k % 2, :, :, :, cols].reshape(owned * cap, width)
            total = lax.dot_general(low_ref[...], block, over, preferred_element_type=jnp.float32)
            total += lax.dot_general(mid_ref[...], block, over, preferred_element_type=jnp.float32)
            out[index, :, cols] = total + lax.dot_general(big_ref[...], block, over, preferred_element_type=jnp.float32)
            return carry
        lax.fori_loop(0, dim // width, part, 0)

    def twin(i):
        return pltpu.make_async_remote_copy(src_ref=pass_ref.at[i % 2], dst_ref=twin_ref.at[i], send_sem=twin_send.at[i],
                                            recv_sem=twin_recv.at[i], device_id={'ep': sibling}, device_id_type=MESH)

    def hop(slot):
        if slot < 2:
            src, dst = sum_ref.at[0, (lows, highs)[slot]], far_ref.at[slot]
        else:
            rows = (lows, highs)[slot % 2]
            src, dst = sum_ref.at[slot // 2, rows], near_ref.at[slot // 2 - 1, rows]
        return pltpu.make_async_remote_copy(src_ref=src, dst_ref=dst, send_sem=send.at[slot], recv_sem=recv.at[slot],
                                            device_id={'ep': (right, left, right, right, left, left)[slot]}, device_id_type=MESH)

    fetch(0).start()
    for i in range(4):
        if i >= 2:
            twin(i - 2).wait_send()
        partial(2 * i, pass_ref, i % 2)
        twin(i).start()
        partial(2 * i + 1, sum_ref, i)
        twin(i).wait_recv()
        sum_ref[i] += twin_ref[i]
        if i == 0:
            hop(0).start()
            hop(1).start()
        if i == 1:
            hop(3).start()
        if i == 2:
            hop(4).start()
    hop(0).wait_recv()
    sum_ref[1, lows] += far_ref[0]
    hop(2).start()
    hop(1).wait_recv()
    sum_ref[2, highs] += far_ref[1]
    hop(5).start()
    sum_ref[3] += h_ref[...].astype(jnp.float32)
    hop(3).wait_recv()
    sum_ref[3, highs] += near_ref[0, highs]
    hop(4).wait_recv()
    sum_ref[3, lows] += near_ref[1, lows]
    hop(2).wait_recv()
    y_ref[lows] = (sum_ref[3, lows] + near_ref[0, lows]).astype(jnp.bfloat16)
    hop(5).wait_recv()
    y_ref[highs] = (sum_ref[3, highs] + near_ref[1, highs]).astype(jnp.bfloat16)
    for i in (2, 3):
        twin(i).wait_send()
    for slot in range(6):
        hop(slot).wait_send()


def settle(mesh_n, table, h, done):
    toks, dim = h.shape
    owned, parts = done.shape[:2]
    bf, f32 = jnp.bfloat16, jnp.float32
    vmem = pl.BlockSpec(memory_space=pltpu.VMEM)
    return pl.pallas_call(
        functools.partial(settle_kernel, mesh_n),
        in_specs=[vmem, vmem, pl.BlockSpec(memory_space=pltpu.HBM)],
        out_specs=vmem,
        out_shape=jax.ShapeDtypeStruct((toks, dim), bf),
        scratch_shapes=[pltpu.VMEM((owned * parts * SLOT, toks), bf)] * 3 + [
            pltpu.VMEM((2, owned, parts, SLOT, dim), bf),
            pltpu.VMEM((2, toks, dim), f32),
            pltpu.VMEM((4, toks, dim), f32),
            pltpu.VMEM((4, toks, dim), f32),
            pltpu.VMEM((2, toks // 2, dim), f32),
            pltpu.VMEM((2, toks, dim), f32),
            pltpu.SemaphoreType.DMA((2,)),
            pltpu.SemaphoreType.DMA((4,)),
            pltpu.SemaphoreType.DMA((4,)),
            pltpu.SemaphoreType.DMA((6,)),
            pltpu.SemaphoreType.DMA((6,)),
        ],
        compiler_params=pltpu.CompilerParams(collective_id=2, has_side_effects=True, vmem_limit_bytes=60 * 2 ** 20),
        cost_estimate=pl.CostEstimate(flops=6 * mesh_n * owned * parts * SLOT * toks * dim, bytes_accessed=60_000_000, transcendentals=0),
        name='settle',
    )(table, h, done)


def solution(mesh):
    tok_spec = P(('dp', 'ep'))
    row_spec = P('ep')
    n = mesh.shape['ep']

    def local_layer(tokens, w_query, w_key, w_value, w_out, w_router, w_one, w_three, w_two, expert_ids):
        seq_count, seq_len, model_dim = tokens.shape
        choices = expert_ids.shape[2]
        experts = w_router.shape[1]
        owned = w_one.shape[0]
        toks = seq_count * seq_len
        parts = 2 * toks * choices // experts // SLOT

        member, slots = slot_table(expert_ids.reshape(toks, choices), experts)
        flat = [w.reshape(w.shape[0], -1) for w in (w_query, w_key, w_value, w_out)]
        hidden = attend(n, seq_len, tokens.reshape(toks, model_dim), *flat)
        normed, gates_local = dense_gates(hidden, w_router, member)
        mine = jnp.concatenate([slots.astype(jnp.float32).T.reshape(n, owned, toks), gates_local.T.reshape(n, owned, toks)], axis=1)
        rows, table = route(n, normed, mine, parts)
        need = jnp.max(table[:, :owned], axis=(0, 2)).astype(jnp.int32) // SLOT + 1
        done = ffn(need, rows, w_one, w_three, w_two)
        layer_out = settle(n, table, hidden, done)
        return layer_out.reshape(seq_count, seq_len, model_dim)

    return jax.shard_map(local_layer, mesh=mesh, in_specs=(tok_spec, row_spec, row_spec, row_spec, row_spec, P(), row_spec, row_spec, row_spec, tok_spec), out_specs=tok_spec, check_vma=False)
```

```python
import functools

import jax
import jax.numpy as jnp
from jax import lax
from jax.experimental import pallas as pl
from jax.experimental.pallas import tpu as pltpu
from jax.sharding import PartitionSpec as P

EPS = 1e-6
SLOT = 16
VMEM_BYTES = 60 * 2 ** 20
ROWS_BY_ROWS = (((1,), (1,)), ((), ()))
TALL_BY_TALL = (((0,), (0,)), ((), ()))
MESH = pl.DeviceIdType.MESH


def neighbours(mesh_n):
    me = lax.axis_index('ep')
    core = me % 2
    sibling = me + 1 - 2 * core
    return me, core, sibling, (me + 2) % mesh_n, (me + mesh_n - 2) % mesh_n, (me + mesh_n // 2) % mesh_n


def meet(mesh_n, me):
    barrier = pltpu.get_barrier_semaphore()
    for j in range(1, mesh_n):
        pl.semaphore_signal(barrier, inc=1, device_id={'ep': (me + j) % mesh_n}, device_id_type=MESH)
    pl.semaphore_wait(barrier, mesh_n - 1)


def attend_kernel(mesh_n, stride, seq_len, x_ref, wq_ref, wk_ref, wv_ref, wo_ref, h_ref, fq_ref, fk_ref, fv_ref, fo_ref,
                  n_ref, q_ref, k_ref, wide_ref, tall_ref, sum_ref, send, recv, load_sem):
    me, core, sibling, right, left, across = neighbours(mesh_n)
    dp = lax.axis_index('dp')
    zbit, ybit = dp % 2, (dp // stride) % 2
    zflip, yflip = dp + 1 - 2 * zbit, dp + stride * (1 - 2 * ybit)
    place = zbit + ybit * (3 - 2 * zbit)
    after = zflip + (place % 2) * (yflip - zflip)
    before = yflip + (place % 2) * (zflip - yflip)
    own_refs = (wq_ref, wk_ref, wv_ref, wo_ref)
    full_refs = (fq_ref, fk_ref, fv_ref, fo_ref)

    barrier = pltpu.get_barrier_semaphore()
    for peer in (right, left, sibling):
        pl.semaphore_signal(barrier, inc=1, device_id={'ep': peer}, device_id_type=MESH)
    for peer in (after, before):
        pl.semaphore_signal(barrier, inc=1, device_id={'dp': peer}, device_id_type=MESH)
    pl.semaphore_wait(barrier, 5)

    def quarter(m, j):
        size = own_refs[m].shape[0] // 4
        return pl.ds(pl.multiple_of((place + j) % 4 * size, size), size)

    def ways(m):
        return (right, left) if m % 2 == 0 else (left, right)

    def sources(m):
        fore, back = ways(m)
        return back, fore, across

    def twin(source):
        return source + 1 - 2 * core

    def copy(m, slot, src, dst, peer):
        return pltpu.make_async_remote_copy(src_ref=src, dst_ref=dst, send_sem=send.at[m, slot], recv_sem=recv.at[m, slot],
                                            device_id=peer, device_id_type=MESH)

    def outgoing(m, slot):
        full, own, (fore, back) = full_refs[m], own_refs[m], ways(m)
        if slot < 4:
            rows = quarter(m, (0, 1, 1, 0)[slot])
            return copy(m, slot, own.at[rows], full.at[me, rows], {'ep': fore if slot < 2 else back})
        if slot == 12:
            return copy(m, slot, own, full.at[me], {'ep': sibling})
        if slot < 6:
            source, rows, peer = (back, fore)[slot - 4], quarter(m, slot - 4), {'ep': (fore, back)[slot - 4]}
        elif slot < 12:
            source, rows, peer = sources(m)[slot % 3], quarter(m, slot // 9), {'dp': after if slot < 9 else before}
        else:
            source, rows, peer = sources(m)[(slot - 13) % 3], quarter(m, (0, 1, 3, 2)[(slot - 13) // 3]), {'ep': sibling}
        return copy(m, slot, full.at[source, rows], full.at[source, rows], peer)

    def arrived(m, slot):
        full, (fore, back) = full_refs[m], ways(m)
        if slot < 4:
            dst = full.at[back if slot < 2 else fore, quarter(m, (0, 1, 1, 0)[slot])]
        elif slot < 6:
            dst = full.at[across, quarter(m, slot - 4)]
        elif slot < 12:
            dst = full.at[sources(m)[slot % 3], quarter(m, 3 if slot < 9 else 2)]
        elif slot == 12:
            dst = full.at[sibling]
        else:
            dst = full.at[twin(sources(m)[(slot - 13) % 3]), quarter(m, (0, 1, 3, 2)[(slot - 13) // 3])]
        copy(m, slot, dst, dst, {'ep': sibling}).wait_recv()

    def start(m, *slots):
        for slot in slots:
            outgoing(m, slot).start()

    def own(m):
        start(m, 0, 2, 1, 3, 12)

    def near_first(m):
        arrived(m, 0)
        start(m, 4, 6, 13)
        arrived(m, 2)
        start(m, 5, 10, 17)

    def near_last(m):
        arrived(m, 1)
        start(m, 9, 16)
        arrived(m, 3)
        start(m, 7, 14)

    def near(m):
        near_first(m)
        near_last(m)

    def far(m):
        arrived(m, 4)
        start(m, 8, 15)
        arrived(m, 5)
        start(m, 11, 18)

    def beside(m, slots=(6, 10, 9, 7, 8, 11)):
        for slot in slots:
            arrived(m, slot)
            start(m, slot + 13)

    def finish(m, slots=tuple(range(12, 25))):
        for slot in slots:
            arrived(m, slot)

    def stream(m, buf, width, body):
        full, mine = full_refs[m], own_refs[m]
        total = full.shape[2] // width
        def cols(c):
            return pl.ds(pl.multiple_of(c * width, width), width)
        def fetch(c, slot):
            pltpu.make_async_copy(mine.at[:, cols(c)], buf.at[slot, me], load_sem.at[slot]).start()
            for j in range(1, mesh_n):
                owner = (me + j) % mesh_n
                pltpu.make_async_copy(full.at[owner, :, cols(c)], buf.at[slot, owner], load_sem.at[slot]).start()
        fetch(0, 0)
        def step(c, carry):
            slot = c % 2
            @pl.when(c + 1 < total)
            def _():
                fetch(c + 1, 1 - slot)
            pltpu.make_async_copy(full.at[:, :, cols(c)], buf.at[slot], load_sem.at[slot]).wait()
            body(cols(c), buf[slot].reshape(full.shape[0] * full.shape[1], width))
            return carry
        lax.fori_loop(0, total, step, 0)

    def project(m, out):
        def body(cols, chunk):
            out[:, cols] = jnp.dot(n_ref[...], chunk, preferred_element_type=jnp.float32).astype(jnp.bfloat16)
        stream(m, wide_ref, wide_ref.shape[3], body)

    head_dim = 128
    seqs = x_ref.shape[0] // seq_len
    causal = lax.broadcasted_iota(jnp.int32, (seq_len, seq_len), 0) >= lax.broadcasted_iota(jnp.int32, (seq_len, seq_len), 1)

    pairs = q_ref.shape[1] // head_dim // 2

    def weigh(first, last):
        def step(i, carry):
            for b in range(seqs):
                rows = slice(b * seq_len, (b + 1) * seq_len)
                for j in range(2):
                    cols = pl.ds(pl.multiple_of((2 * i + j) * head_dim, head_dim), head_dim)
                    scores = lax.dot_general(q_ref[rows, cols], k_ref[rows, cols], ROWS_BY_ROWS,
                                             preferred_element_type=jnp.float32) * head_dim ** -0.5
                    scores = jnp.where(causal, scores, -jnp.inf)
                    grown = jnp.exp(scores - jnp.max(scores, axis=1, keepdims=True))
                    q_ref[rows, cols] = (grown * (1.0 / jnp.sum(grown, axis=1, keepdims=True))).astype(jnp.bfloat16)
            return carry
        lax.fori_loop(first, last, step, 0)

    def mix(cols, chunk):
        values = jnp.dot(n_ref[...], chunk, preferred_element_type=jnp.float32).astype(jnp.bfloat16)
        for j in range(values.shape[1] // head_dim):
            lanes = slice(j * head_dim, (j + 1) * head_dim)
            here = pl.ds(pl.multiple_of(cols.start + j * head_dim, head_dim), head_dim)
            for b in range(seqs):
                rows = slice(b * seq_len, (b + 1) * seq_len)
                q_ref[rows, here] = jnp.dot(q_ref[rows, here], values[rows, lanes], preferred_element_type=jnp.float32).astype(jnp.bfloat16)

    own(0)
    own(1)
    wide = x_ref[...].astype(jnp.float32)
    n_ref[...] = (wide * lax.rsqrt(jnp.mean(wide * wide, axis=-1, keepdims=True) + EPS)).astype(jnp.bfloat16)
    near(0)
    near(1)
    own(2)
    far(0)
    far(1)
    beside(0)
    finish(0)
    project(0, q_ref)
    beside(1)
    finish(1)
    near_first(2)
    own(3)
    project(1, k_ref)
    near_last(2)
    weigh(0, pairs // 2)
    far(2)
    near_first(3)
    weigh(pairs // 2, pairs)
    beside(2)
    finish(2)
    stream(2, wide_ref, wide_ref.shape[3], mix)
    near_last(3)
    far(3)
    late = [slot for slot in range(13, 25) if (slot - 13) % 3 == 2]
    beside(3, (6, 10, 9, 7))
    finish(3, [slot for slot in range(12, 25) if slot not in late])

    fore, back = ways(3)
    depth = fo_ref.shape[1]
    order = (me, sibling, back, fore, twin(back), twin(fore), across, twin(across))
    def fetch(i):
        source = wo_ref if i == 0 else fo_ref.at[order[i]]
        pltpu.make_async_copy(source, tall_ref.at[i % 2], load_sem.at[i % 2]).start()
    def gather_product(first, last):
        fetch(first)
        for i in range(first, last):
            if i + 1 < last:
                fetch(i + 1)
            pltpu.make_async_copy(fo_ref.at[order[i]], tall_ref.at[i % 2], load_sem.at[i % 2]).wait()
            heads = pl.ds(pl.multiple_of(order[i] * depth, depth), depth)
            width = min(512, sum_ref.shape[1])
            def part(c, carry):
                cols = pl.ds(pl.multiple_of(c * width, width), width)
                product = jnp.dot(q_ref[:, heads], tall_ref[i % 2, :, cols], preferred_element_type=jnp.float32)
                if i == 0:
                    sum_ref[:, cols] = x_ref[:, cols].astype(jnp.float32) + product
                elif i < mesh_n - 1:
                    sum_ref[:, cols] += product
                else:
                    h_ref[:, cols] = (sum_ref[:, cols] + product).astype(jnp.bfloat16)
                return carry
            lax.fori_loop(0, sum_ref.shape[1] // width, part, 0)
    gather_product(0, mesh_n - 2)
    beside(3, (8, 11))
    finish(3, late)
    gather_product(mesh_n - 2, mesh_n)
    for m in range(4):
        for slot in range(25):
            outgoing(m, slot).wait_send()


def attend(mesh_n, stride, seq_len, x, wq, wk, wv, wo):
    toks, dim = x.shape
    width = wq.shape[1]
    bf = jnp.bfloat16
    vmem = pl.BlockSpec(memory_space=pltpu.VMEM)
    hbm = pl.BlockSpec(memory_space=pltpu.HBM)
    fulls = [jax.ShapeDtypeStruct((mesh_n,) + w.shape, bf) for w in (wq, wk, wv, wo)]
    out = pl.pallas_call(
        functools.partial(attend_kernel, mesh_n, stride, seq_len),
        in_specs=[vmem, hbm, hbm, hbm, hbm],
        out_specs=[vmem, hbm, hbm, hbm, hbm],
        out_shape=[jax.ShapeDtypeStruct((toks, dim), bf)] + fulls,
        scratch_shapes=[
            pltpu.VMEM((toks, dim), bf),
            pltpu.VMEM((toks, width), bf),
            pltpu.VMEM((toks, width), bf),
            pltpu.VMEM((2, mesh_n, wq.shape[0], min(512, width)), bf),
            pltpu.VMEM((2,) + wo.shape, bf),
            pltpu.VMEM((toks, dim), jnp.float32),
            pltpu.SemaphoreType.DMA((4, 25)),
            pltpu.SemaphoreType.DMA((4, 25)),
            pltpu.SemaphoreType.DMA((2,)),
        ],
        compiler_params=pltpu.CompilerParams(collective_id=0, has_side_effects=True, vmem_limit_bytes=VMEM_BYTES),
        name='attend',
    )(x, wq, wk, wv, wo)
    return out[0]


def route_kernel(mesh_n, h_ref, ids_ref, router_ref, rows_ref, tab_ref, need_ref, u_ref, z_ref, mine_ref, all_ref, hot_ref, stage_ref,
                 send, recv, tab_send, tab_recv, out_sem):
    me, core, sibling, right, left, across = neighbours(mesh_n)
    wide = h_ref[...].astype(jnp.float32)
    z_ref[...] = wide * lax.rsqrt(jnp.mean(wide * wide, axis=-1, keepdims=True) + EPS)
    u_ref[...] = z_ref[...].astype(jnp.bfloat16)
    meet(mesh_n, me)
    toks = u_ref.shape[0]
    half = toks // 2
    lows, highs = pl.ds(0, half), pl.ds(half, half)

    def copy(slot, src, dst, peer):
        return pltpu.make_async_remote_copy(src_ref=src, dst_ref=dst, send_sem=send.at[slot], recv_sem=recv.at[slot],
                                            device_id={'ep': peer}, device_id_type=MESH)

    def outgoing(slot):
        if slot < 4:
            rows = (lows, highs, highs, lows)[slot]
            return copy(slot, u_ref.at[rows], all_ref.at[me, rows], right if slot < 2 else left)
        if slot == 4:
            return copy(slot, all_ref.at[left, lows], all_ref.at[left, lows], right)
        if slot == 5:
            return copy(slot, all_ref.at[right, highs], all_ref.at[right, highs], left)
        if slot == 6:
            return copy(slot, u_ref, all_ref.at[me], sibling)
        if slot < 9:
            source = left if slot == 7 else right
            return copy(slot, all_ref.at[source], all_ref.at[source], sibling)
        rows = lows if slot == 9 else highs
        return copy(slot, all_ref.at[across, rows], all_ref.at[across, rows], sibling)

    def arrived(*slots):
        for slot in slots:
            if slot < 4:
                dst = all_ref.at[left if slot < 2 else right, (lows, highs, highs, lows)[slot]]
            elif slot < 6:
                dst = all_ref.at[across, lows if slot == 4 else highs]
            elif slot == 6:
                dst = all_ref.at[sibling]
            elif slot < 9:
                dst = all_ref.at[(left if slot == 7 else right) + 1 - 2 * core]
            else:
                dst = all_ref.at[across + 1 - 2 * core, lows if slot == 9 else highs]
            copy(slot, dst, dst, sibling).wait_recv()

    def table(j, src, dst, peer):
        return pltpu.make_async_remote_copy(src_ref=src, dst_ref=dst, send_sem=tab_send.at[j], recv_sem=tab_recv.at[j],
                                            device_id={'ep': peer}, device_id_type=MESH)

    def table_out(j):
        peer = (me + j) % mesh_n
        return table(j, mine_ref.at[peer], tab_ref.at[me], peer)

    for slot in (0, 2, 1, 3, 6):
        outgoing(slot).start()
    experts = router_ref.shape[1]
    owned = experts // mesh_n
    index = lax.broadcasted_iota(jnp.int32, (experts, toks), 0)
    member = index == ids_ref[0:1, :]
    for j in range(1, ids_ref.shape[0]):
        member = member | (index == ids_ref[j:j + 1, :])
    earlier = lax.broadcasted_iota(jnp.int32, (toks, toks), 0) < lax.broadcasted_iota(jnp.int32, (toks, toks), 1)
    rank = jnp.dot(jnp.where(member, 1.0, 0.0).astype(jnp.bfloat16), jnp.where(earlier, 1.0, 0.0).astype(jnp.bfloat16),
                   preferred_element_type=jnp.float32)
    slots = jnp.where(member, rank, -1.0)
    logits = lax.dot_general(router_ref[...], z_ref[...], (((0,), (1,)), ((), ())), precision=lax.Precision.HIGHEST,
                             preferred_element_type=jnp.float32)
    top = jnp.max(jnp.where(member, logits, -jnp.inf), axis=0, keepdims=True)
    grown = jnp.where(member, jnp.exp(jnp.where(member, logits, top) - top), 0.0)
    gates = grown / jnp.sum(grown, axis=0, keepdims=True)
    for j in range(mesh_n):
        mine_ref[j, :owned] = slots[j * owned:(j + 1) * owned]
        mine_ref[j, owned:] = gates[j * owned:(j + 1) * owned]
    for j in range(1, mesh_n):
        table_out(j).start()
    tab_ref[me] = mine_ref[me]
    for j in range(1, mesh_n):
        source = (me + mesh_n - j) % mesh_n
        table(j, tab_ref.at[source], tab_ref.at[source], source).wait_recv()
    most = tab_ref[0, :owned]
    for j in range(1, mesh_n):
        most = jnp.maximum(most, tab_ref[j, :owned])
    need_ref[...] = jnp.broadcast_to(jnp.max(most, axis=1, keepdims=True), need_ref.shape)

    parts = rows_ref.shape[1]
    cap = parts * SLOT
    dim = u_ref.shape[1]
    width = min(512, dim)
    lane = lax.broadcasted_iota(jnp.int32, (cap, toks), 0).astype(jnp.float32)

    def flush(k, s):
        return pltpu.make_async_copy(stage_ref.at[k % 2], rows_ref.at[:, :, s], out_sem.at[k % 2])

    def send_rows(k, s, own=False):
        def mark(e, carry):
            pos = tab_ref[s, pl.ds(e, 1)]
            hot_ref[pl.ds(pl.multiple_of(e * cap, SLOT), cap), :] = jnp.where(lane == pos, 1.0, 0.0).astype(jnp.bfloat16)
            return carry
        lax.fori_loop(0, owned, mark, 0)
        if k >= 2:
            flush(k, s).wait()
        def part(c, carry):
            cols = pl.ds(pl.multiple_of(c * width, width), width)
            block = u_ref[:, cols] if own else all_ref[s, :, cols]
            rows = jnp.dot(hot_ref[...], block, preferred_element_type=jnp.float32).astype(jnp.bfloat16)
            stage_ref[k % 2, :, :, :, cols] = rows.reshape(owned, parts, SLOT, width)
            return carry
        lax.fori_loop(0, dim // width, part, 0)
        flush(k, s).start()

    send_rows(0, me, True)
    arrived(6)
    send_rows(1, sibling)
    arrived(0)
    outgoing(4).start()
    arrived(2)
    outgoing(5).start()
    arrived(1)
    outgoing(7).start()
    arrived(3)
    outgoing(8).start()
    send_rows(2, left)
    send_rows(3, right)
    arrived(7)
    send_rows(4, left + 1 - 2 * core)
    arrived(8)
    send_rows(5, right + 1 - 2 * core)
    arrived(4)
    outgoing(9).start()
    arrived(5)
    outgoing(10).start()
    send_rows(6, across)
    arrived(9, 10)
    send_rows(7, across + 1 - 2 * core)
    flush(6, me).wait()
    flush(7, me).wait()
    for j in range(1, mesh_n):
        table_out(j).wait_send()
    for slot in range(11):
        outgoing(slot).wait_send()


def route(mesh_n, h, ids, w_router, parts):
    toks, dim = h.shape
    owned = w_router.shape[1] // mesh_n
    bf, f32 = jnp.bfloat16, jnp.float32
    vmem = pl.BlockSpec(memory_space=pltpu.VMEM)
    return pl.pallas_call(
        functools.partial(route_kernel, mesh_n),
        in_specs=[vmem, vmem, vmem],
        out_specs=[pl.BlockSpec(memory_space=pltpu.HBM), vmem, vmem],
        out_shape=[
            jax.ShapeDtypeStruct((owned, parts, mesh_n, SLOT, dim), bf),
            jax.ShapeDtypeStruct((mesh_n, 2 * owned, toks), f32),
            jax.ShapeDtypeStruct((owned, 128), f32),
        ],
        scratch_shapes=[
            pltpu.VMEM((toks, dim), bf),
            pltpu.VMEM((toks, dim), f32),
            pltpu.VMEM((mesh_n, 2 * owned, toks), f32),
            pltpu.VMEM((mesh_n, toks, dim), bf),
            pltpu.VMEM((owned * parts * SLOT, toks), bf),
            pltpu.VMEM((2, owned, parts, SLOT, dim), bf),
            pltpu.SemaphoreType.DMA((11,)),
            pltpu.SemaphoreType.DMA((11,)),
            pltpu.SemaphoreType.DMA((mesh_n,)),
            pltpu.SemaphoreType.DMA((mesh_n,)),
            pltpu.SemaphoreType.DMA((2,)),
        ],
        compiler_params=pltpu.CompilerParams(collective_id=1, has_side_effects=True, vmem_limit_bytes=VMEM_BYTES),
        name='route',
    )(h, ids, w_router)


def ffn_kernel(need_ref, rows_ref, one_ref, three_ref, two_ref, out_ref):
    parts, n = rows_ref.shape[1], rows_ref.shape[2]
    dim = rows_ref.shape[4]
    step = n * SLOT
    need = need_ref[pl.program_id(0)]
    for used in range(parts + 1):
        @pl.when(need == used)
        def _():
            if used:
                rows = rows_ref[0, :used].reshape(used * step, dim)
                first = jnp.dot(rows, one_ref[0], preferred_element_type=jnp.float32)
                third = jnp.dot(rows, three_ref[0], preferred_element_type=jnp.float32)
                acted = (jax.nn.silu(first) * third).astype(jnp.bfloat16)
                done = jnp.dot(acted, two_ref[0], preferred_element_type=jnp.float32).astype(jnp.bfloat16)
                out_ref[0, :used] = done.reshape(used, n, SLOT, dim)
            if used < parts:
                out_ref[0, used:] = jnp.zeros((parts - used, n, SLOT, dim), jnp.bfloat16)


def ffn(need, rows, w_one, w_three, w_two):
    owned, parts, n, _, dim = rows.shape
    inner = w_one.shape[2]
    tile = pl.BlockSpec((1, parts, n, SLOT, dim), lambda e, _: (e, 0, 0, 0, 0))
    return pl.pallas_call(
        ffn_kernel,
        grid_spec=pltpu.PrefetchScalarGridSpec(
            num_scalar_prefetch=1,
            grid=(owned,),
            in_specs=[
                tile,
                pl.BlockSpec((1, dim, inner), lambda e, _: (e, 0, 0)),
                pl.BlockSpec((1, dim, inner), lambda e, _: (e, 0, 0)),
                pl.BlockSpec((1, inner, dim), lambda e, _: (e, 0, 0)),
            ],
            out_specs=tile,
        ),
        out_shape=jax.ShapeDtypeStruct(rows.shape, jnp.bfloat16),
        compiler_params=pltpu.CompilerParams(vmem_limit_bytes=VMEM_BYTES),
        name="ffn",
    )(need, rows, w_one, w_three, w_two)


def settle_kernel(mesh_n, tab_ref, h_ref, done_ref, y_ref, big_ref, mid_ref, low_ref, load_ref, pass_ref, twin_ref, sum_ref, far_ref, near_ref,
                  load_sem, twin_send, twin_recv, send, recv):
    me, core, sibling, right, left, across = neighbours(mesh_n)
    meet(mesh_n, me)
    toks, dim = h_ref.shape
    half = toks // 2
    lows, highs = slice(0, half), slice(half, toks)
    owned = tab_ref.shape[1] // 2
    parts = done_ref.shape[1]
    cap = parts * SLOT
    width = min(512, dim)
    lane = lax.broadcasted_iota(jnp.int32, (cap, toks), 0).astype(jnp.float32)
    chips = (across, right, left, me)
    jobs = [dest for chip in chips for dest in (chip + 1 - 2 * core, chip)]

    def fetch(k):
        return pltpu.make_async_copy(done_ref.at[:, :, jobs[k]], load_ref.at[k % 2], load_sem.at[k % 2])

    def partial(k, out, index):
        def mark(e, carry):
            here = lane == tab_ref[jobs[k], pl.ds(e, 1)]
            gate = tab_ref[jobs[k], pl.ds(owned + e, 1)]
            big = gate.astype(jnp.bfloat16).astype(jnp.float32)
            mid = (gate - big).astype(jnp.bfloat16).astype(jnp.float32)
            rows = pl.ds(pl.multiple_of(e * cap, SLOT), cap)
            for ref, piece in ((big_ref, big), (mid_ref, mid), (low_ref, (gate - big) - mid)):
                ref[rows, :] = jnp.where(here, piece, 0.0).astype(jnp.bfloat16)
            return carry
        lax.fori_loop(0, owned, mark, 0)
        fetch(k).wait()
        if k + 1 < len(jobs):
            fetch(k + 1).start()
        def part(c, carry):
            cols = pl.ds(pl.multiple_of(c * width, width), width)
            block = load_ref[k % 2, :, :, :, cols].reshape(owned * cap, width)
            total = lax.dot_general(low_ref[...], block, TALL_BY_TALL, preferred_element_type=jnp.float32)
            total += lax.dot_general(mid_ref[...], block, TALL_BY_TALL, preferred_element_type=jnp.float32)
            out[index, :, cols] = total + lax.dot_general(big_ref[...], block, TALL_BY_TALL, preferred_element_type=jnp.float32)
            return carry
        lax.fori_loop(0, dim // width, part, 0)

    def twin(i):
        return pltpu.make_async_remote_copy(src_ref=pass_ref.at[i % 2], dst_ref=twin_ref.at[i], send_sem=twin_send.at[i],
                                            recv_sem=twin_recv.at[i], device_id={'ep': sibling}, device_id_type=MESH)

    def hop(slot):
        if slot < 2:
            src, dst = sum_ref.at[0, (lows, highs)[slot]], far_ref.at[slot]
        else:
            rows = (lows, highs)[slot % 2]
            src, dst = sum_ref.at[slot // 2, rows], near_ref.at[slot // 2 - 1, rows]
        return pltpu.make_async_remote_copy(src_ref=src, dst_ref=dst, send_sem=send.at[slot], recv_sem=recv.at[slot],
                                            device_id={'ep': (right, left, right, right, left, left)[slot]}, device_id_type=MESH)

    fetch(0).start()
    for i in range(4):
        if i >= 2:
            twin(i - 2).wait_send()
        partial(2 * i, pass_ref, i % 2)
        twin(i).start()
        partial(2 * i + 1, sum_ref, i)
        twin(i).wait_recv()
        sum_ref[i] += twin_ref[i]
        if i == 0:
            hop(0).start()
            hop(1).start()
        if i == 1:
            hop(3).start()
        if i == 2:
            hop(4).start()
    hop(0).wait_recv()
    sum_ref[1, lows] += far_ref[0]
    hop(2).start()
    hop(1).wait_recv()
    sum_ref[2, highs] += far_ref[1]
    hop(5).start()
    sum_ref[3] += h_ref[...].astype(jnp.float32)
    hop(3).wait_recv()
    sum_ref[3, highs] += near_ref[0, highs]
    hop(4).wait_recv()
    sum_ref[3, lows] += near_ref[1, lows]
    hop(2).wait_recv()
    y_ref[lows] = (sum_ref[3, lows] + near_ref[0, lows]).astype(jnp.bfloat16)
    hop(5).wait_recv()
    y_ref[highs] = (sum_ref[3, highs] + near_ref[1, highs]).astype(jnp.bfloat16)
    for i in (2, 3):
        twin(i).wait_send()
    for slot in range(6):
        hop(slot).wait_send()


def settle(mesh_n, table, h, done):
    toks, dim = h.shape
    owned, parts = done.shape[:2]
    bf, f32 = jnp.bfloat16, jnp.float32
    vmem = pl.BlockSpec(memory_space=pltpu.VMEM)
    return pl.pallas_call(
        functools.partial(settle_kernel, mesh_n),
        in_specs=[vmem, vmem, pl.BlockSpec(memory_space=pltpu.HBM)],
        out_specs=vmem,
        out_shape=jax.ShapeDtypeStruct((toks, dim), bf),
        scratch_shapes=[pltpu.VMEM((owned * parts * SLOT, toks), bf)] * 3 + [
            pltpu.VMEM((2, owned, parts, SLOT, dim), bf),
            pltpu.VMEM((2, toks, dim), f32),
            pltpu.VMEM((4, toks, dim), f32),
            pltpu.VMEM((4, toks, dim), f32),
            pltpu.VMEM((2, toks // 2, dim), f32),
            pltpu.VMEM((2, toks, dim), f32),
            pltpu.SemaphoreType.DMA((2,)),
            pltpu.SemaphoreType.DMA((4,)),
            pltpu.SemaphoreType.DMA((4,)),
            pltpu.SemaphoreType.DMA((6,)),
            pltpu.SemaphoreType.DMA((6,)),
        ],
        compiler_params=pltpu.CompilerParams(collective_id=2, has_side_effects=True, vmem_limit_bytes=VMEM_BYTES),
        name='settle',
    )(table, h, done)


def solution(mesh):
    tok_spec = P(('dp', 'ep'))
    row_spec = P('ep')
    n = mesh.shape['ep']
    places = [getattr(device, 'coords', None) for device in mesh.devices[:, 0]]
    stride = mesh.shape['dp'] // 2 if places[0] is None else sum(place[1] == places[0][1] for place in places)

    def local_layer(tokens, w_query, w_key, w_value, w_out, w_router, w_one, w_three, w_two, expert_ids):
        seq_count, seq_len, model_dim = tokens.shape
        choices = expert_ids.shape[2]
        experts = w_router.shape[1]
        owned = w_one.shape[0]
        toks = seq_count * seq_len
        parts = 2 * toks * choices // experts // SLOT

        flat = [w.reshape(w.shape[0], -1) for w in (w_query, w_key, w_value, w_out)]
        hidden = attend(n, stride, seq_len, tokens.reshape(toks, model_dim), *flat)
        ids = expert_ids.reshape(toks, choices).T
        rows, table, most = route(n, hidden, ids, w_router, parts)
        need = most[:, 0].astype(jnp.int32) // SLOT + 1
        done = ffn(need, rows, w_one, w_three, w_two)
        layer_out = settle(n, table, hidden, done)
        return layer_out.reshape(seq_count, seq_len, model_dim)

    return jax.shard_map(local_layer, mesh=mesh, in_specs=(tok_spec, row_spec, row_spec, row_spec, row_spec, P(), row_spec, row_spec, row_spec, tok_spec), out_specs=tok_spec, check_vma=False)
```

```python
import functools

import jax
import jax.numpy as jnp
from jax import lax
from jax.experimental import pallas as pl
from jax.experimental.pallas import tpu as pltpu
from jax.sharding import PartitionSpec as P

EPS = 1e-6
SLOT = 16
VMEM_BYTES = 60 * 2 ** 20
ROWS_BY_ROWS = (((1,), (1,)), ((), ()))
TALL_BY_TALL = (((0,), (0,)), ((), ()))
MESH = pl.DeviceIdType.MESH


def neighbours(mesh_n):
    me = lax.axis_index('ep')
    core = me % 2
    sibling = me + 1 - 2 * core
    return me, core, sibling, (me + 2) % mesh_n, (me + mesh_n - 2) % mesh_n, (me + mesh_n // 2) % mesh_n


def meet(mesh_n, me):
    barrier = pltpu.get_barrier_semaphore()
    for j in range(1, mesh_n):
        pl.semaphore_signal(barrier, inc=1, device_id={'ep': (me + j) % mesh_n}, device_id_type=MESH)
    pl.semaphore_wait(barrier, mesh_n - 1)


def attend_kernel(mesh_n, stride, seq_len, x_ref, wq_ref, wk_ref, wv_ref, wo_ref, h_ref, fq_ref, fk_ref, fv_ref, fo_ref,
                  n_ref, q_ref, k_ref, wide_ref, tall_ref, sum_ref, send, recv, load_sem):
    me, core, sibling, right, left, across = neighbours(mesh_n)
    dp = lax.axis_index('dp')
    zbit, ybit = dp % 2, (dp // stride) % 2
    zflip, yflip = dp + 1 - 2 * zbit, dp + stride * (1 - 2 * ybit)
    place = zbit + ybit * (3 - 2 * zbit)
    after = zflip + (place % 2) * (yflip - zflip)
    before = yflip + (place % 2) * (zflip - yflip)
    own_refs = (wq_ref, wk_ref, wv_ref, wo_ref)
    full_refs = (fq_ref, fk_ref, fv_ref, fo_ref)

    barrier = pltpu.get_barrier_semaphore()
    for peer in (right, left, sibling):
        pl.semaphore_signal(barrier, inc=1, device_id={'ep': peer}, device_id_type=MESH)
    for peer in (after, before):
        pl.semaphore_signal(barrier, inc=1, device_id={'dp': peer}, device_id_type=MESH)
    pl.semaphore_wait(barrier, 5)

    def quarter(m, j):
        size = own_refs[m].shape[0] // 4
        return pl.ds(pl.multiple_of((place + j) % 4 * size, size), size)

    def ways(m):
        return (right, left) if m % 2 == 0 else (left, right)

    def sources(m):
        fore, back = ways(m)
        return back, fore, across

    def twin(source):
        return source + 1 - 2 * core

    def copy(m, slot, src, dst, peer):
        return pltpu.make_async_remote_copy(src_ref=src, dst_ref=dst, send_sem=send.at[m, slot], recv_sem=recv.at[m, slot],
                                            device_id=peer, device_id_type=MESH)

    def outgoing(m, slot):
        full, own, (fore, back) = full_refs[m], own_refs[m], ways(m)
        if slot < 4:
            rows = quarter(m, (0, 1, 1, 0)[slot])
            return copy(m, slot, own.at[rows], full.at[me, rows], {'ep': fore if slot < 2 else back})
        if slot == 12:
            return copy(m, slot, own, full.at[me], {'ep': sibling})
        if slot < 6:
            source, rows, peer = (back, fore)[slot - 4], quarter(m, slot - 4), {'ep': (fore, back)[slot - 4]}
        elif slot < 12:
            source, rows, peer = sources(m)[slot % 3], quarter(m, slot // 9), {'dp': after if slot < 9 else before}
        else:
            source, rows, peer = sources(m)[(slot - 13) % 3], quarter(m, (0, 1, 3, 2)[(slot - 13) // 3]), {'ep': sibling}
        return copy(m, slot, full.at[source, rows], full.at[source, rows], peer)

    def arrived(m, slot):
        full, (fore, back) = full_refs[m], ways(m)
        if slot < 4:
            dst = full.at[back if slot < 2 else fore, quarter(m, (0, 1, 1, 0)[slot])]
        elif slot < 6:
            dst = full.at[across, quarter(m, slot - 4)]
        elif slot < 12:
            dst = full.at[sources(m)[slot % 3], quarter(m, 3 if slot < 9 else 2)]
        elif slot == 12:
            dst = full.at[sibling]
        else:
            dst = full.at[twin(sources(m)[(slot - 13) % 3]), quarter(m, (0, 1, 3, 2)[(slot - 13) // 3])]
        copy(m, slot, dst, dst, {'ep': sibling}).wait_recv()

    def start(m, *slots):
        for slot in slots:
            outgoing(m, slot).start()

    def own(m):
        start(m, 0, 2, 1, 3, 12)

    def near_first(m):
        arrived(m, 0)
        start(m, 4, 6, 13)
        arrived(m, 2)
        start(m, 5, 10, 17)

    def near_last(m):
        arrived(m, 1)
        start(m, 9, 16)
        arrived(m, 3)
        start(m, 7, 14)

    def near(m):
        near_first(m)
        near_last(m)

    def far(m):
        arrived(m, 4)
        start(m, 8, 15)
        arrived(m, 5)
        start(m, 11, 18)

    def beside(m, slots=(6, 10, 9, 7, 8, 11)):
        for slot in slots:
            arrived(m, slot)
            start(m, slot + 13)

    def finish(m, slots=tuple(range(12, 25))):
        for slot in slots:
            arrived(m, slot)

    def stream(m, buf, width, body):
        full, mine = full_refs[m], own_refs[m]
        total = full.shape[2] // width
        def cols(c):
            return pl.ds(pl.multiple_of(c * width, width), width)
        def fetch(c, slot):
            pltpu.make_async_copy(mine.at[:, cols(c)], buf.at[slot, me], load_sem.at[slot]).start()
            for j in range(1, mesh_n):
                owner = (me + j) % mesh_n
                pltpu.make_async_copy(full.at[owner, :, cols(c)], buf.at[slot, owner], load_sem.at[slot]).start()
        fetch(0, 0)
        def step(c, carry):
            slot = c % 2
            @pl.when(c + 1 < total)
            def _():
                fetch(c + 1, 1 - slot)
            pltpu.make_async_copy(full.at[:, :, cols(c)], buf.at[slot], load_sem.at[slot]).wait()
            body(cols(c), buf[slot].reshape(full.shape[0] * full.shape[1], width))
            return carry
        lax.fori_loop(0, total, step, 0)

    def project(m, out):
        def body(cols, chunk):
            out[:, cols] = jnp.dot(n_ref[...], chunk, preferred_element_type=jnp.float32).astype(jnp.bfloat16)
        stream(m, wide_ref, wide_ref.shape[3], body)

    head_dim = 128
    seqs = x_ref.shape[0] // seq_len
    causal = lax.broadcasted_iota(jnp.int32, (seq_len, seq_len), 0) >= lax.broadcasted_iota(jnp.int32, (seq_len, seq_len), 1)

    pairs = q_ref.shape[1] // head_dim // 2

    def weigh(first, last):
        def step(i, carry):
            for b in range(seqs):
                rows = slice(b * seq_len, (b + 1) * seq_len)
                for j in range(2):
                    cols = pl.ds(pl.multiple_of((2 * i + j) * head_dim, head_dim), head_dim)
                    scores = lax.dot_general(q_ref[rows, cols], k_ref[rows, cols], ROWS_BY_ROWS,
                                             preferred_element_type=jnp.float32) * head_dim ** -0.5
                    scores = jnp.where(causal, scores, -jnp.inf)
                    grown = jnp.exp(scores - jnp.max(scores, axis=1, keepdims=True))
                    q_ref[rows, cols] = (grown * (1.0 / jnp.sum(grown, axis=1, keepdims=True))).astype(jnp.bfloat16)
            return carry
        lax.fori_loop(first, last, step, 0)

    def mix(cols, chunk):
        values = jnp.dot(n_ref[...], chunk, preferred_element_type=jnp.float32).astype(jnp.bfloat16)
        for j in range(values.shape[1] // head_dim):
            lanes = slice(j * head_dim, (j + 1) * head_dim)
            here = pl.ds(pl.multiple_of(cols.start + j * head_dim, head_dim), head_dim)
            for b in range(seqs):
                rows = slice(b * seq_len, (b + 1) * seq_len)
                q_ref[rows, here] = jnp.dot(q_ref[rows, here], values[rows, lanes], preferred_element_type=jnp.float32).astype(jnp.bfloat16)

    own(0)
    own(1)
    wide = x_ref[...].astype(jnp.float32)
    n_ref[...] = (wide * lax.rsqrt(jnp.mean(wide * wide, axis=-1, keepdims=True) + EPS)).astype(jnp.bfloat16)
    near(0)
    near(1)
    own(2)
    far(0)
    far(1)
    beside(0)
    finish(0)
    project(0, q_ref)
    beside(1)
    finish(1)
    near_first(2)
    own(3)
    project(1, k_ref)
    near_last(2)
    weigh(0, pairs // 2)
    far(2)
    near_first(3)
    weigh(pairs // 2, pairs)
    beside(2)
    finish(2)
    stream(2, wide_ref, wide_ref.shape[3], mix)
    near_last(3)
    far(3)
    late = [slot for slot in range(13, 25) if (slot - 13) % 3 == 2]
    beside(3, (6, 10, 9, 7))
    finish(3, [slot for slot in range(12, 25) if slot not in late])

    fore, back = ways(3)
    depth = fo_ref.shape[1]
    order = (me, sibling, back, fore, twin(back), twin(fore), across, twin(across))
    def fetch(i):
        source = wo_ref if i == 0 else fo_ref.at[order[i]]
        pltpu.make_async_copy(source, tall_ref.at[i % 2], load_sem.at[i % 2]).start()
    def gather_product(first, last):
        fetch(first)
        for i in range(first, last):
            if i + 1 < last:
                fetch(i + 1)
            pltpu.make_async_copy(fo_ref.at[order[i]], tall_ref.at[i % 2], load_sem.at[i % 2]).wait()
            heads = pl.ds(pl.multiple_of(order[i] * depth, depth), depth)
            width = min(512, sum_ref.shape[1])
            def part(c, carry):
                cols = pl.ds(pl.multiple_of(c * width, width), width)
                product = jnp.dot(q_ref[:, heads], tall_ref[i % 2, :, cols], preferred_element_type=jnp.float32)
                if i == 0:
                    sum_ref[:, cols] = x_ref[:, cols].astype(jnp.float32) + product
                elif i < mesh_n - 1:
                    sum_ref[:, cols] += product
                else:
                    h_ref[:, cols] = (sum_ref[:, cols] + product).astype(jnp.bfloat16)
                return carry
            lax.fori_loop(0, sum_ref.shape[1] // width, part, 0)
    gather_product(0, mesh_n - 2)
    beside(3, (8, 11))
    finish(3, late)
    gather_product(mesh_n - 2, mesh_n)
    for m in range(4):
        for slot in range(25):
            outgoing(m, slot).wait_send()


def attend(mesh_n, stride, seq_len, x, wq, wk, wv, wo):
    toks, dim = x.shape
    width = wq.shape[1]
    bf = jnp.bfloat16
    vmem = pl.BlockSpec(memory_space=pltpu.VMEM)
    hbm = pl.BlockSpec(memory_space=pltpu.HBM)
    fulls = [jax.ShapeDtypeStruct((mesh_n,) + w.shape, bf) for w in (wq, wk, wv, wo)]
    out = pl.pallas_call(
        functools.partial(attend_kernel, mesh_n, stride, seq_len),
        in_specs=[vmem, hbm, hbm, hbm, hbm],
        out_specs=[vmem, hbm, hbm, hbm, hbm],
        out_shape=[jax.ShapeDtypeStruct((toks, dim), bf)] + fulls,
        scratch_shapes=[
            pltpu.VMEM((toks, dim), bf),
            pltpu.VMEM((toks, width), bf),
            pltpu.VMEM((toks, width), bf),
            pltpu.VMEM((2, mesh_n, wq.shape[0], min(512, width)), bf),
            pltpu.VMEM((2,) + wo.shape, bf),
            pltpu.VMEM((toks, dim), jnp.float32),
            pltpu.SemaphoreType.DMA((4, 25)),
            pltpu.SemaphoreType.DMA((4, 25)),
            pltpu.SemaphoreType.DMA((2,)),
        ],
        compiler_params=pltpu.CompilerParams(collective_id=0, has_side_effects=True, vmem_limit_bytes=VMEM_BYTES),
        name='attend',
    )(x, wq, wk, wv, wo)
    return out[0]


def route_kernel(mesh_n, h_ref, ids_ref, router_ref, rows_ref, tab_ref, need_ref, u_ref, z_ref, mine_ref, all_ref, hot_ref, stage_ref,
                 send, recv, tab_send, tab_recv, out_sem):
    me, core, sibling, right, left, across = neighbours(mesh_n)
    wide = h_ref[...].astype(jnp.float32)
    z_ref[...] = wide * lax.rsqrt(jnp.mean(wide * wide, axis=-1, keepdims=True) + EPS)
    u_ref[...] = z_ref[...].astype(jnp.bfloat16)
    meet(mesh_n, me)
    toks = u_ref.shape[0]
    half = toks // 2
    lows, highs = pl.ds(0, half), pl.ds(half, half)

    def copy(slot, src, dst, peer):
        return pltpu.make_async_remote_copy(src_ref=src, dst_ref=dst, send_sem=send.at[slot], recv_sem=recv.at[slot],
                                            device_id={'ep': peer}, device_id_type=MESH)

    def outgoing(slot):
        if slot < 4:
            rows = (lows, highs, highs, lows)[slot]
            return copy(slot, u_ref.at[rows], all_ref.at[me, rows], right if slot < 2 else left)
        if slot == 4:
            return copy(slot, all_ref.at[left, lows], all_ref.at[left, lows], right)
        if slot == 5:
            return copy(slot, all_ref.at[right, highs], all_ref.at[right, highs], left)
        if slot == 6:
            return copy(slot, u_ref, all_ref.at[me], sibling)
        if slot < 9:
            source = left if slot == 7 else right
            return copy(slot, all_ref.at[source], all_ref.at[source], sibling)
        rows = lows if slot == 9 else highs
        return copy(slot, all_ref.at[across, rows], all_ref.at[across, rows], sibling)

    def arrived(*slots):
        for slot in slots:
            if slot < 4:
                dst = all_ref.at[left if slot < 2 else right, (lows, highs, highs, lows)[slot]]
            elif slot < 6:
                dst = all_ref.at[across, lows if slot == 4 else highs]
            elif slot == 6:
                dst = all_ref.at[sibling]
            elif slot < 9:
                dst = all_ref.at[(left if slot == 7 else right) + 1 - 2 * core]
            else:
                dst = all_ref.at[across + 1 - 2 * core, lows if slot == 9 else highs]
            copy(slot, dst, dst, sibling).wait_recv()

    def table(j, src, dst, peer):
        return pltpu.make_async_remote_copy(src_ref=src, dst_ref=dst, send_sem=tab_send.at[j], recv_sem=tab_recv.at[j],
                                            device_id={'ep': peer}, device_id_type=MESH)

    def table_out(j):
        peer = (me + j) % mesh_n
        return table(j, mine_ref.at[peer], tab_ref.at[me], peer)

    for slot in (0, 2, 1, 3, 6):
        outgoing(slot).start()
    experts = router_ref.shape[1]
    owned = experts // mesh_n
    index = lax.broadcasted_iota(jnp.int32, (experts, toks), 0)
    member = index == ids_ref[0:1, :]
    for j in range(1, ids_ref.shape[0]):
        member = member | (index == ids_ref[j:j + 1, :])
    earlier = lax.broadcasted_iota(jnp.int32, (toks, toks), 0) < lax.broadcasted_iota(jnp.int32, (toks, toks), 1)
    rank = jnp.dot(jnp.where(member, 1.0, 0.0).astype(jnp.bfloat16), jnp.where(earlier, 1.0, 0.0).astype(jnp.bfloat16),
                   preferred_element_type=jnp.float32)
    slots = jnp.where(member, rank, -1.0)
    logits = lax.dot_general(router_ref[...], z_ref[...], (((0,), (1,)), ((), ())), precision=lax.Precision.HIGHEST,
                             preferred_element_type=jnp.float32)
    top = jnp.max(jnp.where(member, logits, -jnp.inf), axis=0, keepdims=True)
    grown = jnp.where(member, jnp.exp(jnp.where(member, logits, top) - top), 0.0)
    gates = grown / jnp.sum(grown, axis=0, keepdims=True)
    for j in range(mesh_n):
        mine_ref[j, :owned] = slots[j * owned:(j + 1) * owned]
        mine_ref[j, owned:] = gates[j * owned:(j + 1) * owned]
    for j in range(1, mesh_n):
        table_out(j).start()
    tab_ref[me] = mine_ref[me]
    for j in range(1, mesh_n):
        source = (me + mesh_n - j) % mesh_n
        table(j, tab_ref.at[source], tab_ref.at[source], source).wait_recv()
    most = tab_ref[0, :owned]
    for j in range(1, mesh_n):
        most = jnp.maximum(most, tab_ref[j, :owned])
    need_ref[...] = jnp.broadcast_to(jnp.max(most, axis=1, keepdims=True), need_ref.shape)

    parts = rows_ref.shape[1]
    cap = parts * SLOT
    dim = u_ref.shape[1]
    width = min(512, dim)
    lane = lax.broadcasted_iota(jnp.int32, (cap, toks), 0).astype(jnp.float32)

    def flush(k, s):
        return pltpu.make_async_copy(stage_ref.at[k % 2], rows_ref.at[:, :, s], out_sem.at[k % 2])

    def send_rows(k, s, own=False):
        def mark(e, carry):
            pos = tab_ref[s, pl.ds(e, 1)]
            hot_ref[pl.ds(pl.multiple_of(e * cap, SLOT), cap), :] = jnp.where(lane == pos, 1.0, 0.0).astype(jnp.bfloat16)
            return carry
        lax.fori_loop(0, owned, mark, 0)
        if k >= 2:
            flush(k, s).wait()
        def part(c, carry):
            cols = pl.ds(pl.multiple_of(c * width, width), width)
            block = u_ref[:, cols] if own else all_ref[s, :, cols]
            rows = jnp.dot(hot_ref[...], block, preferred_element_type=jnp.float32).astype(jnp.bfloat16)
            stage_ref[k % 2, :, :, :, cols] = rows.reshape(owned, parts, SLOT, width)
            return carry
        lax.fori_loop(0, dim // width, part, 0)
        flush(k, s).start()

    send_rows(0, me, True)
    arrived(6)
    send_rows(1, sibling)
    arrived(0)
    outgoing(4).start()
    arrived(2)
    outgoing(5).start()
    arrived(1)
    outgoing(7).start()
    arrived(3)
    outgoing(8).start()
    send_rows(2, left)
    send_rows(3, right)
    arrived(7)
    send_rows(4, left + 1 - 2 * core)
    arrived(8)
    send_rows(5, right + 1 - 2 * core)
    arrived(4)
    outgoing(9).start()
    arrived(5)
    outgoing(10).start()
    send_rows(6, across)
    arrived(9, 10)
    send_rows(7, across + 1 - 2 * core)
    flush(6, me).wait()
    flush(7, me).wait()
    for j in range(1, mesh_n):
        table_out(j).wait_send()
    for slot in range(11):
        outgoing(slot).wait_send()


def route(mesh_n, h, ids, w_router, parts):
    toks, dim = h.shape
    owned = w_router.shape[1] // mesh_n
    bf, f32 = jnp.bfloat16, jnp.float32
    vmem = pl.BlockSpec(memory_space=pltpu.VMEM)
    return pl.pallas_call(
        functools.partial(route_kernel, mesh_n),
        in_specs=[vmem, vmem, vmem],
        out_specs=[pl.BlockSpec(memory_space=pltpu.HBM), vmem, vmem],
        out_shape=[
            jax.ShapeDtypeStruct((owned, parts, mesh_n, SLOT, dim), bf),
            jax.ShapeDtypeStruct((mesh_n, 2 * owned, toks), f32),
            jax.ShapeDtypeStruct((owned, 128), f32),
        ],
        scratch_shapes=[
            pltpu.VMEM((toks, dim), bf),
            pltpu.VMEM((toks, dim), f32),
            pltpu.VMEM((mesh_n, 2 * owned, toks), f32),
            pltpu.VMEM((mesh_n, toks, dim), bf),
            pltpu.VMEM((owned * parts * SLOT, toks), bf),
            pltpu.VMEM((2, owned, parts, SLOT, dim), bf),
            pltpu.SemaphoreType.DMA((11,)),
            pltpu.SemaphoreType.DMA((11,)),
            pltpu.SemaphoreType.DMA((mesh_n,)),
            pltpu.SemaphoreType.DMA((mesh_n,)),
            pltpu.SemaphoreType.DMA((2,)),
        ],
        compiler_params=pltpu.CompilerParams(collective_id=1, has_side_effects=True, vmem_limit_bytes=VMEM_BYTES),
        name='route',
    )(h, ids, w_router)


def ffn_kernel(most_ref, rows_ref, one_ref, three_ref, two_ref, out_ref, in_buf, one_buf, three_buf, two_buf, out_buf, load_sem, part_sem, out_sem):
    owned, parts, n, _, dim = rows_ref.shape
    depth = one_buf.shape[0]
    step = n * SLOT

    def need(e):
        return most_ref[e, 0].astype(jnp.int32) // SLOT + 1

    def loads(e, act):
        slot = e % depth
        for i, (src, buf) in enumerate(((one_ref, one_buf), (three_ref, three_buf), (two_ref, two_buf))):
            act(pltpu.make_async_copy(src.at[e], buf.at[slot], load_sem.at[slot, i]))
        for p in range(parts):
            @pl.when(p < need(e))
            def _():
                act(pltpu.make_async_copy(rows_ref.at[e, p], in_buf.at[slot, p], part_sem.at[slot, p]))

    def store(e):
        return pltpu.make_async_copy(out_buf.at[e % 2], out_ref.at[e], out_sem.at[e % 2])

    def begin(copy):
        copy.start()

    def end(copy):
        copy.wait()

    for e in range(depth):
        loads(e, begin)

    def expert(e, carry):
        slot, place, count = e % depth, e % 2, need(e)
        loads(e, end)
        @pl.when(e > 1)
        def _():
            store(e).wait()
        for used in range(1, parts + 1):
            @pl.when(count == used)
            def _():
                rows = in_buf[slot, :used].reshape(used * step, dim)
                first = jnp.dot(rows, one_buf[slot], preferred_element_type=jnp.float32)
                third = jnp.dot(rows, three_buf[slot], preferred_element_type=jnp.float32)
                acted = (jax.nn.silu(first) * third).astype(jnp.bfloat16)
                done = jnp.dot(acted, two_buf[slot], preferred_element_type=jnp.float32).astype(jnp.bfloat16)
                out_buf[place, :used] = done.reshape(used, n, SLOT, dim)
                if used < parts:
                    out_buf[place, used:] = jnp.zeros((parts - used, n, SLOT, dim), jnp.bfloat16)
        store(e).start()
        @pl.when(e + depth < owned)
        def _():
            loads(e + depth, begin)
        return carry
    lax.fori_loop(0, owned, expert, 0)
    for e in range(owned - 2, owned):
        store(e).wait()


def ffn(most, rows, w_one, w_three, w_two):
    owned, parts, n, _, dim = rows.shape
    depth = min(3, owned)
    hbm = pl.BlockSpec(memory_space=pltpu.HBM)
    return pl.pallas_call(
        ffn_kernel,
        in_specs=[pl.BlockSpec(memory_space=pltpu.SMEM)] + [hbm] * 4,
        out_specs=hbm,
        out_shape=jax.ShapeDtypeStruct(rows.shape, jnp.bfloat16),
        scratch_shapes=[pltpu.VMEM((depth,) + rows.shape[1:], jnp.bfloat16)]
        + [pltpu.VMEM((depth,) + w.shape[1:], jnp.bfloat16) for w in (w_one, w_three, w_two)]
        + [
            pltpu.VMEM((2,) + rows.shape[1:], jnp.bfloat16),
            pltpu.SemaphoreType.DMA((depth, 3)),
            pltpu.SemaphoreType.DMA((depth, parts)),
            pltpu.SemaphoreType.DMA((2,)),
        ],
        compiler_params=pltpu.CompilerParams(vmem_limit_bytes=VMEM_BYTES),
        name='ffn',
    )(most, rows, w_one, w_three, w_two)


def settle_kernel(mesh_n, tab_ref, h_ref, done_ref, y_ref, big_ref, mid_ref, low_ref, load_ref, pass_ref, twin_ref, sum_ref, far_ref, near_ref,
                  load_sem, twin_send, twin_recv, send, recv):
    me, core, sibling, right, left, across = neighbours(mesh_n)
    meet(mesh_n, me)
    toks, dim = h_ref.shape
    half = toks // 2
    lows, highs = slice(0, half), slice(half, toks)
    owned = tab_ref.shape[1] // 2
    parts = done_ref.shape[1]
    cap = parts * SLOT
    width = min(512, dim)
    lane = lax.broadcasted_iota(jnp.int32, (cap, toks), 0).astype(jnp.float32)
    chips = (across, right, left, me)
    jobs = [dest for chip in chips for dest in (chip + 1 - 2 * core, chip)]

    def fetch(k):
        return pltpu.make_async_copy(done_ref.at[:, :, jobs[k]], load_ref.at[k % 2], load_sem.at[k % 2])

    def partial(k, out, index):
        def mark(e, carry):
            here = lane == tab_ref[jobs[k], pl.ds(e, 1)]
            gate = tab_ref[jobs[k], pl.ds(owned + e, 1)]
            big = gate.astype(jnp.bfloat16).astype(jnp.float32)
            mid = (gate - big).astype(jnp.bfloat16).astype(jnp.float32)
            rows = pl.ds(pl.multiple_of(e * cap, SLOT), cap)
            for ref, piece in ((big_ref, big), (mid_ref, mid), (low_ref, (gate - big) - mid)):
                ref[rows, :] = jnp.where(here, piece, 0.0).astype(jnp.bfloat16)
            return carry
        lax.fori_loop(0, owned, mark, 0)
        fetch(k).wait()
        if k + 1 < len(jobs):
            fetch(k + 1).start()
        def part(c, carry):
            cols = pl.ds(pl.multiple_of(c * width, width), width)
            block = load_ref[k % 2, :, :, :, cols].reshape(owned * cap, width)
            total = lax.dot_general(low_ref[...], block, TALL_BY_TALL, preferred_element_type=jnp.float32)
            total += lax.dot_general(mid_ref[...], block, TALL_BY_TALL, preferred_element_type=jnp.float32)
            out[index, :, cols] = total + lax.dot_general(big_ref[...], block, TALL_BY_TALL, preferred_element_type=jnp.float32)
            return carry
        lax.fori_loop(0, dim // width, part, 0)

    def twin(i):
        return pltpu.make_async_remote_copy(src_ref=pass_ref.at[i % 2], dst_ref=twin_ref.at[i], send_sem=twin_send.at[i],
                                            recv_sem=twin_recv.at[i], device_id={'ep': sibling}, device_id_type=MESH)

    def hop(slot):
        if slot < 2:
            src, dst = sum_ref.at[0, (lows, highs)[slot]], far_ref.at[slot]
        else:
            rows = (lows, highs)[slot % 2]
            src, dst = sum_ref.at[slot // 2, rows], near_ref.at[slot // 2 - 1, rows]
        return pltpu.make_async_remote_copy(src_ref=src, dst_ref=dst, send_sem=send.at[slot], recv_sem=recv.at[slot],
                                            device_id={'ep': (right, left, right, right, left, left)[slot]}, device_id_type=MESH)

    fetch(0).start()
    for i in range(4):
        if i >= 2:
            twin(i - 2).wait_send()
        partial(2 * i, pass_ref, i % 2)
        twin(i).start()
        partial(2 * i + 1, sum_ref, i)
        twin(i).wait_recv()
        sum_ref[i] += twin_ref[i]
        if i == 0:
            hop(0).start()
            hop(1).start()
        if i == 1:
            hop(3).start()
        if i == 2:
            hop(4).start()
    hop(0).wait_recv()
    sum_ref[1, lows] += far_ref[0]
    hop(2).start()
    hop(1).wait_recv()
    sum_ref[2, highs] += far_ref[1]
    hop(5).start()
    sum_ref[3] += h_ref[...].astype(jnp.float32)
    hop(3).wait_recv()
    sum_ref[3, highs] += near_ref[0, highs]
    hop(4).wait_recv()
    sum_ref[3, lows] += near_ref[1, lows]
    hop(2).wait_recv()
    y_ref[lows] = (sum_ref[3, lows] + near_ref[0, lows]).astype(jnp.bfloat16)
    hop(5).wait_recv()
    y_ref[highs] = (sum_ref[3, highs] + near_ref[1, highs]).astype(jnp.bfloat16)
    for i in (2, 3):
        twin(i).wait_send()
    for slot in range(6):
        hop(slot).wait_send()


def settle(mesh_n, table, h, done):
    toks, dim = h.shape
    owned, parts = done.shape[:2]
    bf, f32 = jnp.bfloat16, jnp.float32
    vmem = pl.BlockSpec(memory_space=pltpu.VMEM)
    return pl.pallas_call(
        functools.partial(settle_kernel, mesh_n),
        in_specs=[vmem, vmem, pl.BlockSpec(memory_space=pltpu.HBM)],
        out_specs=vmem,
        out_shape=jax.ShapeDtypeStruct((toks, dim), bf),
        scratch_shapes=[pltpu.VMEM((owned * parts * SLOT, toks), bf)] * 3 + [
            pltpu.VMEM((2, owned, parts, SLOT, dim), bf),
            pltpu.VMEM((2, toks, dim), f32),
            pltpu.VMEM((4, toks, dim), f32),
            pltpu.VMEM((4, toks, dim), f32),
            pltpu.VMEM((2, toks // 2, dim), f32),
            pltpu.VMEM((2, toks, dim), f32),
            pltpu.SemaphoreType.DMA((2,)),
            pltpu.SemaphoreType.DMA((4,)),
            pltpu.SemaphoreType.DMA((4,)),
            pltpu.SemaphoreType.DMA((6,)),
            pltpu.SemaphoreType.DMA((6,)),
        ],
        compiler_params=pltpu.CompilerParams(collective_id=2, has_side_effects=True, vmem_limit_bytes=VMEM_BYTES),
        name='settle',
    )(table, h, done)


def solution(mesh):
    tok_spec = P(('dp', 'ep'))
    row_spec = P('ep')
    n = mesh.shape['ep']
    places = [getattr(device, 'coords', None) for device in mesh.devices[:, 0]]
    stride = mesh.shape['dp'] // 2 if places[0] is None else sum(place[1] == places[0][1] for place in places)

    def local_layer(tokens, w_query, w_key, w_value, w_out, w_router, w_one, w_three, w_two, expert_ids):
        seq_count, seq_len, model_dim = tokens.shape
        choices = expert_ids.shape[2]
        experts = w_router.shape[1]
        owned = w_one.shape[0]
        toks = seq_count * seq_len
        parts = 2 * toks * choices // experts // SLOT

        flat = [w.reshape(w.shape[0], -1) for w in (w_query, w_key, w_value, w_out)]
        hidden = attend(n, stride, seq_len, tokens.reshape(toks, model_dim), *flat)
        ids = expert_ids.reshape(toks, choices).T
        rows, table, most = route(n, hidden, ids, w_router, parts)
        done = ffn(most, rows, w_one, w_three, w_two)
        layer_out = settle(n, table, hidden, done)
        return layer_out.reshape(seq_count, seq_len, model_dim)

    return jax.shard_map(local_layer, mesh=mesh, in_specs=(tok_spec, row_spec, row_spec, row_spec, row_spec, P(), row_spec, row_spec, row_spec, tok_spec), out_specs=tok_spec, check_vma=False)
```

```python
import functools

import jax
import jax.numpy as jnp
from jax import lax
from jax.experimental import pallas as pl
from jax.experimental.pallas import tpu as pltpu
from jax.sharding import PartitionSpec as P

EPS = 1e-6
SLOT = 16
VMEM_BYTES = 60 * 2 ** 20
ROWS_BY_ROWS = (((1,), (1,)), ((), ()))
TALL_BY_TALL = (((0,), (0,)), ((), ()))
MESH = pl.DeviceIdType.MESH


def neighbours(mesh_n):
    me = lax.axis_index('ep')
    core = me % 2
    sibling = me + 1 - 2 * core
    return me, core, sibling, (me + 2) % mesh_n, (me + mesh_n - 2) % mesh_n, (me + mesh_n // 2) % mesh_n


def greet(mesh_n, me):
    for j in range(1, mesh_n):
        pl.semaphore_signal(pltpu.get_barrier_semaphore(), inc=1, device_id={'ep': (me + j) % mesh_n}, device_id_type=MESH)


def meet(mesh_n):
    pl.semaphore_wait(pltpu.get_barrier_semaphore(), mesh_n - 1)


def attend_kernel(mesh_n, stride, seq_len, x_ref, wq_ref, wk_ref, wv_ref, wo_ref, h_ref, fq_ref, fk_ref, fv_ref, fo_ref,
                  n_ref, q_ref, k_ref, wide_ref, tall_ref, sum_ref, send, recv, load_sem):
    me, core, sibling, right, left, across = neighbours(mesh_n)
    dp = lax.axis_index('dp')
    zbit, ybit = dp % 2, (dp // stride) % 2
    zflip, yflip = dp + 1 - 2 * zbit, dp + stride * (1 - 2 * ybit)
    place = zbit + ybit * (3 - 2 * zbit)
    after = zflip + (place % 2) * (yflip - zflip)
    before = yflip + (place % 2) * (zflip - yflip)
    own_refs = (wq_ref, wk_ref, wv_ref, wo_ref)
    full_refs = (fq_ref, fk_ref, fv_ref, fo_ref)

    barrier = pltpu.get_barrier_semaphore()
    for peer in (right, left, sibling):
        pl.semaphore_signal(barrier, inc=1, device_id={'ep': peer}, device_id_type=MESH)
    for peer in (after, before):
        pl.semaphore_signal(barrier, inc=1, device_id={'dp': peer}, device_id_type=MESH)
    pl.semaphore_wait(barrier, 5)

    def quarter(m, j):
        size = own_refs[m].shape[0] // 4
        return pl.ds(pl.multiple_of((place + j) % 4 * size, size), size)

    def ways(m):
        return (right, left) if m % 2 == 0 else (left, right)

    def sources(m):
        fore, back = ways(m)
        return back, fore, across

    def twin(source):
        return source + 1 - 2 * core

    def copy(m, slot, src, dst, peer):
        return pltpu.make_async_remote_copy(src_ref=src, dst_ref=dst, send_sem=send.at[m, slot], recv_sem=recv.at[m, slot],
                                            device_id=peer, device_id_type=MESH)

    def outgoing(m, slot):
        full, own, (fore, back) = full_refs[m], own_refs[m], ways(m)
        if slot < 4:
            rows = quarter(m, (0, 1, 1, 0)[slot])
            return copy(m, slot, own.at[rows], full.at[me, rows], {'ep': fore if slot < 2 else back})
        if slot == 12:
            return copy(m, slot, own, full.at[me], {'ep': sibling})
        if slot < 6:
            source, rows, peer = (back, fore)[slot - 4], quarter(m, slot - 4), {'ep': (fore, back)[slot - 4]}
        elif slot < 12:
            source, rows, peer = sources(m)[slot % 3], quarter(m, slot // 9), {'dp': after if slot < 9 else before}
        else:
            source, rows, peer = sources(m)[(slot - 13) % 3], quarter(m, (0, 1, 3, 2)[(slot - 13) // 3]), {'ep': sibling}
        return copy(m, slot, full.at[source, rows], full.at[source, rows], peer)

    def arrived(m, slot):
        full, (fore, back) = full_refs[m], ways(m)
        if slot < 4:
            dst = full.at[back if slot < 2 else fore, quarter(m, (0, 1, 1, 0)[slot])]
        elif slot < 6:
            dst = full.at[across, quarter(m, slot - 4)]
        elif slot < 12:
            dst = full.at[sources(m)[slot % 3], quarter(m, 3 if slot < 9 else 2)]
        elif slot == 12:
            dst = full.at[sibling]
        else:
            dst = full.at[twin(sources(m)[(slot - 13) % 3]), quarter(m, (0, 1, 3, 2)[(slot - 13) // 3])]
        copy(m, slot, dst, dst, {'ep': sibling}).wait_recv()

    def start(m, *slots):
        for slot in slots:
            outgoing(m, slot).start()

    def own(m):
        start(m, 0, 2, 1, 3, 12)

    def near_first(m):
        arrived(m, 0)
        start(m, 4, 6, 13)
        arrived(m, 2)
        start(m, 5, 10, 17)

    def near_last(m):
        arrived(m, 1)
        start(m, 9, 16)
        arrived(m, 3)
        start(m, 7, 14)

    def near(m):
        near_first(m)
        near_last(m)

    def far(m):
        arrived(m, 4)
        start(m, 8, 15)
        arrived(m, 5)
        start(m, 11, 18)

    def beside(m, slots=(6, 10, 9, 7, 8, 11)):
        for slot in slots:
            arrived(m, slot)
            start(m, slot + 13)

    def finish(m, slots=tuple(range(12, 25))):
        for slot in slots:
            arrived(m, slot)

    def stream(m, buf, width, body):
        full, mine = full_refs[m], own_refs[m]
        total = full.shape[2] // width
        def cols(c):
            return pl.ds(pl.multiple_of(c * width, width), width)
        def fetch(c, slot):
            pltpu.make_async_copy(mine.at[:, cols(c)], buf.at[slot, me], load_sem.at[slot]).start()
            for j in range(1, mesh_n):
                owner = (me + j) % mesh_n
                pltpu.make_async_copy(full.at[owner, :, cols(c)], buf.at[slot, owner], load_sem.at[slot]).start()
        fetch(0, 0)
        def step(c, carry):
            slot = c % 2
            @pl.when(c + 1 < total)
            def _():
                fetch(c + 1, 1 - slot)
            pltpu.make_async_copy(full.at[:, :, cols(c)], buf.at[slot], load_sem.at[slot]).wait()
            body(cols(c), buf[slot].reshape(full.shape[0] * full.shape[1], width))
            return carry
        lax.fori_loop(0, total, step, 0)

    def project(m, out):
        def body(cols, chunk):
            out[:, cols] = jnp.dot(n_ref[...], chunk, preferred_element_type=jnp.float32).astype(jnp.bfloat16)
        stream(m, wide_ref, wide_ref.shape[3], body)

    head_dim = 128
    seqs = x_ref.shape[0] // seq_len
    causal = lax.broadcasted_iota(jnp.int32, (seq_len, seq_len), 0) >= lax.broadcasted_iota(jnp.int32, (seq_len, seq_len), 1)

    pairs = q_ref.shape[1] // head_dim // 2

    def weigh(first, last):
        def step(i, carry):
            for b in range(seqs):
                rows = slice(b * seq_len, (b + 1) * seq_len)
                for j in range(2):
                    cols = pl.ds(pl.multiple_of((2 * i + j) * head_dim, head_dim), head_dim)
                    scores = lax.dot_general(q_ref[rows, cols], k_ref[rows, cols], ROWS_BY_ROWS,
                                             preferred_element_type=jnp.float32) * head_dim ** -0.5
                    scores = jnp.where(causal, scores, -jnp.inf)
                    grown = jnp.exp(scores - jnp.max(scores, axis=1, keepdims=True))
                    q_ref[rows, cols] = (grown * (1.0 / jnp.sum(grown, axis=1, keepdims=True))).astype(jnp.bfloat16)
            return carry
        lax.fori_loop(first, last, step, 0)

    def mix(cols, chunk):
        values = jnp.dot(n_ref[...], chunk, preferred_element_type=jnp.float32).astype(jnp.bfloat16)
        for j in range(values.shape[1] // head_dim):
            lanes = slice(j * head_dim, (j + 1) * head_dim)
            here = pl.ds(pl.multiple_of(cols.start + j * head_dim, head_dim), head_dim)
            for b in range(seqs):
                rows = slice(b * seq_len, (b + 1) * seq_len)
                q_ref[rows, here] = jnp.dot(q_ref[rows, here], values[rows, lanes], preferred_element_type=jnp.float32).astype(jnp.bfloat16)

    own(0)
    own(1)
    wide = x_ref[...].astype(jnp.float32)
    n_ref[...] = (wide * lax.rsqrt(jnp.mean(wide * wide, axis=-1, keepdims=True) + EPS)).astype(jnp.bfloat16)
    near(0)
    near(1)
    own(2)
    far(0)
    far(1)
    beside(0)
    finish(0)
    project(0, q_ref)
    beside(1)
    finish(1)
    near_first(2)
    own(3)
    project(1, k_ref)
    near_last(2)
    weigh(0, pairs // 2)
    far(2)
    near_first(3)
    weigh(pairs // 2, pairs)
    beside(2)
    finish(2)
    stream(2, wide_ref, wide_ref.shape[3], mix)
    near_last(3)
    far(3)
    late = [slot for slot in range(13, 25) if (slot - 13) % 3 == 2]
    beside(3, (6, 10, 9, 7))
    finish(3, [slot for slot in range(12, 25) if slot not in late])

    fore, back = ways(3)
    depth = fo_ref.shape[1]
    order = (me, sibling, back, fore, twin(back), twin(fore), across, twin(across))
    def fetch(i):
        source = wo_ref if i == 0 else fo_ref.at[order[i]]
        pltpu.make_async_copy(source, tall_ref.at[i % 2], load_sem.at[i % 2]).start()
    def gather_product(first, last):
        fetch(first)
        for i in range(first, last):
            if i + 1 < last:
                fetch(i + 1)
            pltpu.make_async_copy(fo_ref.at[order[i]], tall_ref.at[i % 2], load_sem.at[i % 2]).wait()
            heads = pl.ds(pl.multiple_of(order[i] * depth, depth), depth)
            width = min(512, sum_ref.shape[1])
            def part(c, carry):
                cols = pl.ds(pl.multiple_of(c * width, width), width)
                product = jnp.dot(q_ref[:, heads], tall_ref[i % 2, :, cols], preferred_element_type=jnp.float32)
                if i == 0:
                    sum_ref[:, cols] = x_ref[:, cols].astype(jnp.float32) + product
                elif i < mesh_n - 1:
                    sum_ref[:, cols] += product
                else:
                    h_ref[:, cols] = (sum_ref[:, cols] + product).astype(jnp.bfloat16)
                return carry
            lax.fori_loop(0, sum_ref.shape[1] // width, part, 0)
    gather_product(0, mesh_n - 2)
    beside(3, (8, 11))
    finish(3, late)
    gather_product(mesh_n - 2, mesh_n)
    for m in range(4):
        for slot in range(25):
            outgoing(m, slot).wait_send()


def attend(mesh_n, stride, seq_len, x, wq, wk, wv, wo):
    toks, dim = x.shape
    width = wq.shape[1]
    bf = jnp.bfloat16
    vmem = pl.BlockSpec(memory_space=pltpu.VMEM)
    hbm = pl.BlockSpec(memory_space=pltpu.HBM)
    fulls = [jax.ShapeDtypeStruct((mesh_n,) + w.shape, bf) for w in (wq, wk, wv, wo)]
    out = pl.pallas_call(
        functools.partial(attend_kernel, mesh_n, stride, seq_len),
        in_specs=[vmem, hbm, hbm, hbm, hbm],
        out_specs=[vmem, hbm, hbm, hbm, hbm],
        out_shape=[jax.ShapeDtypeStruct((toks, dim), bf)] + fulls,
        scratch_shapes=[
            pltpu.VMEM((toks, dim), bf),
            pltpu.VMEM((toks, width), bf),
            pltpu.VMEM((toks, width), bf),
            pltpu.VMEM((2, mesh_n, wq.shape[0], min(512, width)), bf),
            pltpu.VMEM((2,) + wo.shape, bf),
            pltpu.VMEM((toks, dim), jnp.float32),
            pltpu.SemaphoreType.DMA((4, 25)),
            pltpu.SemaphoreType.DMA((4, 25)),
            pltpu.SemaphoreType.DMA((2,)),
        ],
        compiler_params=pltpu.CompilerParams(collective_id=0, has_side_effects=True, vmem_limit_bytes=VMEM_BYTES),
        name='attend',
    )(x, wq, wk, wv, wo)
    return out[0]


def route_kernel(mesh_n, h_ref, ids_ref, router_ref, rows_ref, tab_ref, need_ref, u_ref, z_ref, mine_ref, all_ref, hot_ref, stage_ref,
                 send, recv, tab_send, tab_recv, out_sem):
    me, core, sibling, right, left, across = neighbours(mesh_n)
    greet(mesh_n, me)
    wide = h_ref[...].astype(jnp.float32)
    z_ref[...] = wide * lax.rsqrt(jnp.mean(wide * wide, axis=-1, keepdims=True) + EPS)
    u_ref[...] = z_ref[...].astype(jnp.bfloat16)
    meet(mesh_n)
    toks = u_ref.shape[0]
    half = toks // 2
    lows, highs = pl.ds(0, half), pl.ds(half, half)

    def copy(slot, src, dst, peer):
        return pltpu.make_async_remote_copy(src_ref=src, dst_ref=dst, send_sem=send.at[slot], recv_sem=recv.at[slot],
                                            device_id={'ep': peer}, device_id_type=MESH)

    def outgoing(slot):
        if slot < 4:
            rows = (lows, highs, highs, lows)[slot]
            return copy(slot, u_ref.at[rows], all_ref.at[me, rows], right if slot < 2 else left)
        if slot == 4:
            return copy(slot, all_ref.at[left, lows], all_ref.at[left, lows], right)
        if slot == 5:
            return copy(slot, all_ref.at[right, highs], all_ref.at[right, highs], left)
        if slot == 6:
            return copy(slot, u_ref, all_ref.at[me], sibling)
        if slot < 9:
            source = left if slot == 7 else right
            return copy(slot, all_ref.at[source], all_ref.at[source], sibling)
        rows = lows if slot == 9 else highs
        return copy(slot, all_ref.at[across, rows], all_ref.at[across, rows], sibling)

    def arrived(*slots):
        for slot in slots:
            if slot < 4:
                dst = all_ref.at[left if slot < 2 else right, (lows, highs, highs, lows)[slot]]
            elif slot < 6:
                dst = all_ref.at[across, lows if slot == 4 else highs]
            elif slot == 6:
                dst = all_ref.at[sibling]
            elif slot < 9:
                dst = all_ref.at[(left if slot == 7 else right) + 1 - 2 * core]
            else:
                dst = all_ref.at[across + 1 - 2 * core, lows if slot == 9 else highs]
            copy(slot, dst, dst, sibling).wait_recv()

    def table(j, src, dst, peer):
        return pltpu.make_async_remote_copy(src_ref=src, dst_ref=dst, send_sem=tab_send.at[j], recv_sem=tab_recv.at[j],
                                            device_id={'ep': peer}, device_id_type=MESH)

    def table_out(j):
        peer = (me + j) % mesh_n
        return table(j, mine_ref.at[peer], tab_ref.at[me], peer)

    for slot in (0, 2, 1, 3, 6):
        outgoing(slot).start()
    experts = router_ref.shape[1]
    owned = experts // mesh_n
    index = lax.broadcasted_iota(jnp.int32, (experts, toks), 0)
    member = index == ids_ref[0:1, :]
    for j in range(1, ids_ref.shape[0]):
        member = member | (index == ids_ref[j:j + 1, :])
    earlier = lax.broadcasted_iota(jnp.int32, (toks, toks), 0) < lax.broadcasted_iota(jnp.int32, (toks, toks), 1)
    rank = jnp.dot(jnp.where(member, 1.0, 0.0).astype(jnp.bfloat16), jnp.where(earlier, 1.0, 0.0).astype(jnp.bfloat16),
                   preferred_element_type=jnp.float32)
    slots = jnp.where(member, rank, -1.0)
    logits = lax.dot_general(router_ref[...], z_ref[...], (((0,), (1,)), ((), ())), precision=lax.Precision.HIGHEST,
                             preferred_element_type=jnp.float32)
    top = jnp.max(jnp.where(member, logits, -jnp.inf), axis=0, keepdims=True)
    grown = jnp.where(member, jnp.exp(jnp.where(member, logits, top) - top), 0.0)
    gates = grown / jnp.sum(grown, axis=0, keepdims=True)
    for j in range(mesh_n):
        mine_ref[j, :owned] = slots[j * owned:(j + 1) * owned]
        mine_ref[j, owned:] = gates[j * owned:(j + 1) * owned]
    for j in range(1, mesh_n):
        table_out(j).start()
    tab_ref[me] = mine_ref[me]
    for j in range(1, mesh_n):
        source = (me + mesh_n - j) % mesh_n
        table(j, tab_ref.at[source], tab_ref.at[source], source).wait_recv()
    most = tab_ref[0, :owned]
    for j in range(1, mesh_n):
        most = jnp.maximum(most, tab_ref[j, :owned])
    need_ref[...] = jnp.broadcast_to(jnp.max(most, axis=1, keepdims=True), need_ref.shape)

    parts = rows_ref.shape[1]
    cap = parts * SLOT
    dim = u_ref.shape[1]
    width = min(512, dim)
    lane = lax.broadcasted_iota(jnp.int32, (cap, toks), 0).astype(jnp.float32)

    def flush(k, s):
        return pltpu.make_async_copy(stage_ref.at[k % 2], rows_ref.at[:, :, s], out_sem.at[k % 2])

    def send_rows(k, s, own=False):
        def mark(e, carry):
            pos = tab_ref[s, pl.ds(e, 1)]
            hot_ref[pl.ds(pl.multiple_of(e * cap, SLOT), cap), :] = jnp.where(lane == pos, 1.0, 0.0).astype(jnp.bfloat16)
            return carry
        lax.fori_loop(0, owned, mark, 0)
        if k >= 2:
            flush(k, s).wait()
        def part(c, carry):
            cols = pl.ds(pl.multiple_of(c * width, width), width)
            block = u_ref[:, cols] if own else all_ref[s, :, cols]
            rows = jnp.dot(hot_ref[...], block, preferred_element_type=jnp.float32).astype(jnp.bfloat16)
            stage_ref[k % 2, :, :, :, cols] = rows.reshape(owned, parts, SLOT, width)
            return carry
        lax.fori_loop(0, dim // width, part, 0)
        flush(k, s).start()

    send_rows(0, me, True)
    arrived(6)
    send_rows(1, sibling)
    arrived(0)
    outgoing(4).start()
    arrived(2)
    outgoing(5).start()
    arrived(1)
    outgoing(7).start()
    arrived(3)
    outgoing(8).start()
    send_rows(2, left)
    send_rows(3, right)
    arrived(7)
    send_rows(4, left + 1 - 2 * core)
    arrived(8)
    send_rows(5, right + 1 - 2 * core)
    arrived(4)
    outgoing(9).start()
    arrived(5)
    outgoing(10).start()
    send_rows(6, across)
    arrived(9, 10)
    send_rows(7, across + 1 - 2 * core)
    flush(6, me).wait()
    flush(7, me).wait()
    for j in range(1, mesh_n):
        table_out(j).wait_send()
    for slot in range(11):
        outgoing(slot).wait_send()


def route(mesh_n, h, ids, w_router, parts):
    toks, dim = h.shape
    owned = w_router.shape[1] // mesh_n
    bf, f32 = jnp.bfloat16, jnp.float32
    vmem = pl.BlockSpec(memory_space=pltpu.VMEM)
    return pl.pallas_call(
        functools.partial(route_kernel, mesh_n),
        in_specs=[vmem, vmem, vmem],
        out_specs=[pl.BlockSpec(memory_space=pltpu.HBM), vmem, vmem],
        out_shape=[
            jax.ShapeDtypeStruct((owned, parts, mesh_n, SLOT, dim), bf),
            jax.ShapeDtypeStruct((mesh_n, 2 * owned, toks), f32),
            jax.ShapeDtypeStruct((owned, 128), f32),
        ],
        scratch_shapes=[
            pltpu.VMEM((toks, dim), bf),
            pltpu.VMEM((toks, dim), f32),
            pltpu.VMEM((mesh_n, 2 * owned, toks), f32),
            pltpu.VMEM((mesh_n, toks, dim), bf),
            pltpu.VMEM((owned * parts * SLOT, toks), bf),
            pltpu.VMEM((2, owned, parts, SLOT, dim), bf),
            pltpu.SemaphoreType.DMA((11,)),
            pltpu.SemaphoreType.DMA((11,)),
            pltpu.SemaphoreType.DMA((mesh_n,)),
            pltpu.SemaphoreType.DMA((mesh_n,)),
            pltpu.SemaphoreType.DMA((2,)),
        ],
        compiler_params=pltpu.CompilerParams(collective_id=1, has_side_effects=True, vmem_limit_bytes=VMEM_BYTES),
        name='route',
    )(h, ids, w_router)


def ffn_kernel(most_ref, rows_ref, one_ref, three_ref, two_ref, out_ref, in_buf, one_buf, three_buf, two_buf, out_buf, load_sem, part_sem, out_sem):
    owned, parts, n, _, dim = rows_ref.shape
    depth = one_buf.shape[0]
    step = n * SLOT

    def need(e):
        return most_ref[e, 0].astype(jnp.int32) // SLOT + 1

    def loads(e, act):
        slot = e % depth
        for i, (src, buf) in enumerate(((one_ref, one_buf), (three_ref, three_buf), (two_ref, two_buf))):
            act(pltpu.make_async_copy(src.at[e], buf.at[slot], load_sem.at[slot, i]))
        for p in range(parts):
            @pl.when(p < need(e))
            def _():
                act(pltpu.make_async_copy(rows_ref.at[e, p], in_buf.at[slot, p], part_sem.at[slot, p]))

    def store(e):
        return pltpu.make_async_copy(out_buf.at[e % 2], out_ref.at[e], out_sem.at[e % 2])

    def begin(copy):
        copy.start()

    def end(copy):
        copy.wait()

    for e in range(depth):
        loads(e, begin)

    def expert(e, carry):
        slot, place, count = e % depth, e % 2, need(e)
        loads(e, end)
        @pl.when(e > 1)
        def _():
            store(e).wait()
        for used in range(1, parts + 1):
            @pl.when(count == used)
            def _():
                rows = in_buf[slot, :used].reshape(used * step, dim)
                first = jnp.dot(rows, one_buf[slot], preferred_element_type=jnp.float32)
                third = jnp.dot(rows, three_buf[slot], preferred_element_type=jnp.float32)
                acted = (jax.nn.silu(first) * third).astype(jnp.bfloat16)
                done = jnp.dot(acted, two_buf[slot], preferred_element_type=jnp.float32).astype(jnp.bfloat16)
                out_buf[place, :used] = done.reshape(used, n, SLOT, dim)
                if used < parts:
                    out_buf[place, used:] = jnp.zeros((parts - used, n, SLOT, dim), jnp.bfloat16)
        store(e).start()
        @pl.when(e + depth < owned)
        def _():
            loads(e + depth, begin)
        return carry
    lax.fori_loop(0, owned, expert, 0)
    for e in range(owned - 2, owned):
        store(e).wait()


def ffn(most, rows, w_one, w_three, w_two):
    owned, parts, n, _, dim = rows.shape
    depth = min(4, owned)
    hbm = pl.BlockSpec(memory_space=pltpu.HBM)
    return pl.pallas_call(
        ffn_kernel,
        in_specs=[pl.BlockSpec(memory_space=pltpu.SMEM)] + [hbm] * 4,
        out_specs=hbm,
        out_shape=jax.ShapeDtypeStruct(rows.shape, jnp.bfloat16),
        scratch_shapes=[pltpu.VMEM((depth,) + rows.shape[1:], jnp.bfloat16)]
        + [pltpu.VMEM((depth,) + w.shape[1:], jnp.bfloat16) for w in (w_one, w_three, w_two)]
        + [
            pltpu.VMEM((2,) + rows.shape[1:], jnp.bfloat16),
            pltpu.SemaphoreType.DMA((depth, 3)),
            pltpu.SemaphoreType.DMA((depth, parts)),
            pltpu.SemaphoreType.DMA((2,)),
        ],
        compiler_params=pltpu.CompilerParams(vmem_limit_bytes=VMEM_BYTES),
        name='ffn',
    )(most, rows, w_one, w_three, w_two)


def settle_kernel(mesh_n, tab_ref, h_ref, done_ref, y_ref, big_ref, mid_ref, low_ref, load_ref, pass_ref, twin_ref, sum_ref, far_ref, near_ref,
                  load_sem, twin_send, twin_recv, send, recv):
    me, core, sibling, right, left, across = neighbours(mesh_n)
    greet(mesh_n, me)
    toks, dim = h_ref.shape
    half = toks // 2
    lows, highs = slice(0, half), slice(half, toks)
    owned = tab_ref.shape[1] // 2
    parts = done_ref.shape[1]
    cap = parts * SLOT
    width = min(512, dim)
    lane = lax.broadcasted_iota(jnp.int32, (cap, toks), 0).astype(jnp.float32)
    chips = (across, right, left, me)
    jobs = [dest for chip in chips for dest in (chip + 1 - 2 * core, chip)]

    def fetch(k):
        return pltpu.make_async_copy(done_ref.at[:, :, jobs[k]], load_ref.at[k % 2], load_sem.at[k % 2])

    def partial(k, out, index):
        def mark(e, carry):
            here = lane == tab_ref[jobs[k], pl.ds(e, 1)]
            gate = tab_ref[jobs[k], pl.ds(owned + e, 1)]
            big = gate.astype(jnp.bfloat16).astype(jnp.float32)
            mid = (gate - big).astype(jnp.bfloat16).astype(jnp.float32)
            rows = pl.ds(pl.multiple_of(e * cap, SLOT), cap)
            for ref, piece in ((big_ref, big), (mid_ref, mid), (low_ref, (gate - big) - mid)):
                ref[rows, :] = jnp.where(here, piece, 0.0).astype(jnp.bfloat16)
            return carry
        lax.fori_loop(0, owned, mark, 0)
        fetch(k).wait()
        if k + 1 < len(jobs):
            fetch(k + 1).start()
        def part(c, carry):
            cols = pl.ds(pl.multiple_of(c * width, width), width)
            block = load_ref[k % 2, :, :, :, cols].reshape(owned * cap, width)
            total = lax.dot_general(low_ref[...], block, TALL_BY_TALL, preferred_element_type=jnp.float32)
            total += lax.dot_general(mid_ref[...], block, TALL_BY_TALL, preferred_element_type=jnp.float32)
            out[index, :, cols] = total + lax.dot_general(big_ref[...], block, TALL_BY_TALL, preferred_element_type=jnp.float32)
            return carry
        lax.fori_loop(0, dim // width, part, 0)

    def twin(i):
        return pltpu.make_async_remote_copy(src_ref=pass_ref.at[i % 2], dst_ref=twin_ref.at[i], send_sem=twin_send.at[i],
                                            recv_sem=twin_recv.at[i], device_id={'ep': sibling}, device_id_type=MESH)

    def hop(slot):
        if slot < 2:
            src, dst = sum_ref.at[0, (lows, highs)[slot]], far_ref.at[slot]
        else:
            rows = (lows, highs)[slot % 2]
            src, dst = sum_ref.at[slot // 2, rows], near_ref.at[slot // 2 - 1, rows]
        return pltpu.make_async_remote_copy(src_ref=src, dst_ref=dst, send_sem=send.at[slot], recv_sem=recv.at[slot],
                                            device_id={'ep': (right, left, right, right, left, left)[slot]}, device_id_type=MESH)

    fetch(0).start()
    for i in range(4):
        if i >= 2:
            twin(i - 2).wait_send()
        partial(2 * i, pass_ref, i % 2)
        if i == 0:
            meet(mesh_n)
        twin(i).start()
        partial(2 * i + 1, sum_ref, i)
        twin(i).wait_recv()
        sum_ref[i] += twin_ref[i]
        if i == 0:
            hop(0).start()
            hop(1).start()
        if i == 1:
            hop(3).start()
        if i == 2:
            hop(4).start()
    hop(0).wait_recv()
    sum_ref[1, lows] += far_ref[0]
    hop(2).start()
    hop(1).wait_recv()
    sum_ref[2, highs] += far_ref[1]
    hop(5).start()
    sum_ref[3] += h_ref[...].astype(jnp.float32)
    hop(3).wait_recv()
    sum_ref[3, highs] += near_ref[0, highs]
    hop(4).wait_recv()
    sum_ref[3, lows] += near_ref[1, lows]
    hop(2).wait_recv()
    y_ref[lows] = (sum_ref[3, lows] + near_ref[0, lows]).astype(jnp.bfloat16)
    hop(5).wait_recv()
    y_ref[highs] = (sum_ref[3, highs] + near_ref[1, highs]).astype(jnp.bfloat16)
    for i in (2, 3):
        twin(i).wait_send()
    for slot in range(6):
        hop(slot).wait_send()


def settle(mesh_n, table, h, done):
    toks, dim = h.shape
    owned, parts = done.shape[:2]
    bf, f32 = jnp.bfloat16, jnp.float32
    vmem = pl.BlockSpec(memory_space=pltpu.VMEM)
    return pl.pallas_call(
        functools.partial(settle_kernel, mesh_n),
        in_specs=[vmem, vmem, pl.BlockSpec(memory_space=pltpu.HBM)],
        out_specs=vmem,
        out_shape=jax.ShapeDtypeStruct((toks, dim), bf),
        scratch_shapes=[pltpu.VMEM((owned * parts * SLOT, toks), bf)] * 3 + [
            pltpu.VMEM((2, owned, parts, SLOT, dim), bf),
            pltpu.VMEM((2, toks, dim), f32),
            pltpu.VMEM((4, toks, dim), f32),
            pltpu.VMEM((4, toks, dim), f32),
            pltpu.VMEM((2, toks // 2, dim), f32),
            pltpu.VMEM((2, toks, dim), f32),
            pltpu.SemaphoreType.DMA((2,)),
            pltpu.SemaphoreType.DMA((4,)),
            pltpu.SemaphoreType.DMA((4,)),
            pltpu.SemaphoreType.DMA((6,)),
            pltpu.SemaphoreType.DMA((6,)),
        ],
        compiler_params=pltpu.CompilerParams(collective_id=2, has_side_effects=True, vmem_limit_bytes=VMEM_BYTES),
        name='settle',
    )(table, h, done)


def solution(mesh):
    tok_spec = P(('dp', 'ep'))
    row_spec = P('ep')
    n = mesh.shape['ep']
    places = [getattr(device, 'coords', None) for device in mesh.devices[:, 0]]
    stride = mesh.shape['dp'] // 2 if places[0] is None else sum(place[1] == places[0][1] for place in places)

    def local_layer(tokens, w_query, w_key, w_value, w_out, w_router, w_one, w_three, w_two, expert_ids):
        seq_count, seq_len, model_dim = tokens.shape
        choices = expert_ids.shape[2]
        experts = w_router.shape[1]
        owned = w_one.shape[0]
        toks = seq_count * seq_len
        parts = 2 * toks * choices // experts // SLOT

        flat = [w.reshape(w.shape[0], -1) for w in (w_query, w_key, w_value, w_out)]
        hidden = attend(n, stride, seq_len, tokens.reshape(toks, model_dim), *flat)
        ids = expert_ids.reshape(toks, choices).T
        rows, table, most = route(n, hidden, ids, w_router, parts)
        done = ffn(most, rows, w_one, w_three, w_two)
        layer_out = settle(n, table, hidden, done)
        return layer_out.reshape(seq_count, seq_len, model_dim)

    return jax.shard_map(local_layer, mesh=mesh, in_specs=(tok_spec, row_spec, row_spec, row_spec, row_spec, P(), row_spec, row_spec, row_spec, tok_spec), out_specs=tok_spec, check_vma=False)
```
